8 devices in a mesh: rep: 1 (over z), r: 2 (over y), s: 4 (over x, core).
Axes of the slice: x: 2, y: 2, z: 1, core: 2. Of those that a mesh axis runs over, the one named last changes fastest.
Arguments:
- x: bfloat16 [8, 4096, 896], P(('rep', 'r', 's'))
- dy: bfloat16 [8, 4096, 896], P(('rep', 'r', 's'))
- w_gate: bfloat16 [2, 896, 2304], P(None, 's')
- w_up: bfloat16 [2, 896, 2304], P(None, 's')
- w_down: bfloat16 [2, 2304, 896], P(None, 's')
- m_w_gate: float32 [2, 896, 2304], P(None, 's')
- m_w_up: float32 [2, 896, 2304], P(None, 's')
- m_w_down: float32 [2, 2304, 896], P(None, 's')
- v_w_gate: float32 [2, 896, 2304], P(None, 's')
- v_w_up: float32 [2, 896, 2304], P(None, 's')
- v_w_down: float32 [2, 2304, 896], P(None, 's')
Outputs:
- output 1: bfloat16 [2, 896, 2304], P('rep', 's')
- output 2: bfloat16 [2, 896, 2304], P('rep', 's')
- output 3: bfloat16 [2, 2304, 896], P('rep', 's')
- output 4: float32 [2, 896, 2304], P('rep', 's')
- output 5: float32 [2, 896, 2304], P('rep', 's')
- output 6: float32 [2, 2304, 896], P('rep', 's')
- output 7: float32 [2, 896, 2304], P('rep', 's')
- output 8: float32 [2, 896, 2304], P('rep', 's')
- output 9: float32 [2, 2304, 896], P('rep', 's')
All inputs are finite; a program needn't handle non-finite values.
Results may differ from the reference program's by a relative error of at most 0.022.
Values are sent between devices in bfloat16 or wider.
A program may use at most 2 GiB of HBM per device.

```python
import jax
import jax.numpy as jnp
from jax import lax

SEQUENCES = 8
TOKENS = 4096
D = 896
FF = 2304
LAYERS = 2
NAMES = ("w_gate", "w_up", "w_down")
SHAPES = {"w_gate": (LAYERS, D, FF), "w_up": (LAYERS, D, FF), "w_down": (LAYERS, FF, D)}


def bump(key, n, height):
    away = (jnp.arange(n, dtype=jnp.int32) - jax.random.randint(key, (), 0, n, jnp.int32)) % n
    return jnp.where(away < n // 8, height, 1.0)


def together(key, own, strength):
    shared = jax.random.normal(key, own.shape[1:], jnp.float32)
    return (own + strength * shared) * lax.rsqrt(1 + strength * strength)


def setup_inputs(seed: int = 0, part: int = 0) -> dict:
    kx, kdy, ka, kb, kz, kf, kh, kl, *keys = jax.random.split(jax.random.key(seed), 8 + 3 * len(NAMES))
    kx, kdy, ka, kb = (jax.random.fold_in(k, part) for k in (kx, kdy, ka, kb))
    kw, km, kv = (keys[i::3] for i in range(3))
    shape = (SEQUENCES, TOKENS, D)
    much_x, much_dy = jax.random.uniform(kz, (2,), jnp.float32, 0.0, 1.0)
    loud = 2.0 ** jax.random.uniform(jax.random.fold_in(kz, 1), (), jnp.float32, -1.0, 2.0)
    layers = 2.0 ** jax.random.uniform(kl, (LAYERS, 1, 1), jnp.float32, -1.0, 1.0)
    x = together(ka, jax.random.normal(kx, shape, jnp.float32), much_x) * bump(kf, D, 4.0)
    dy = together(kb, jax.random.normal(kdy, shape, jnp.float32), much_dy)
    drawn = {"x": x.astype(jnp.bfloat16), "dy": (loud * dy * (SEQUENCES * TOKENS) ** -0.5).astype(jnp.bfloat16)}
    for key, name in zip(kw, NAMES, strict=True):
        w = jax.random.normal(key, SHAPES[name], jnp.float32) * SHAPES[name][1] ** -0.5
        drawn[name] = (w * {"w_gate": 1.0, "w_up": bump(kh, FF, 4.0), "w_down": layers}[name]).astype(jnp.bfloat16)
    for key, name in zip(km, NAMES, strict=True):
        drawn[f"m_{name}"] = 0.1 * jax.random.normal(key, SHAPES[name], jnp.float32)
    for key, name in zip(kv, NAMES, strict=True):
        drawn[f"v_{name}"] = jax.random.uniform(key, SHAPES[name], jnp.float32, 0.005, 0.015)
    return drawn


def matmul(a, w):
    return jnp.dot(a, w, preferred_element_type=jnp.float32).astype(jnp.bfloat16)


def normed(h):
    wide = h.astype(jnp.float32)
    scale = lax.rsqrt(jnp.mean(wide**2, -1, keepdims=True) + 1e-6)
    return (wide * scale).astype(jnp.bfloat16)


def layer(h, w):
    a = normed(h)
    gate = jnp.dot(a, w["w_gate"], preferred_element_type=jnp.float32)
    up = jnp.dot(a, w["w_up"], preferred_element_type=jnp.float32)
    return h + matmul((jax.nn.silu(gate) * up).astype(jnp.bfloat16), w["w_down"])


def adamw(w, m, v, g):
    m = 0.9 * m + 0.1 * g
    v = 0.95 * v + 0.05 * g * g
    step = m * lax.rsqrt(v + 1e-8) + 0.1 * w
    return (w - 0.02 * step).astype(jnp.bfloat16), m, v


def clipped(gradients, sum_of_squares, count):
    factor = jnp.minimum(1.0, 0.5 * lax.rsqrt(sum_of_squares / count + 1e-30))
    return [g * factor for g in gradients]


def stack(weights, h):
    return lax.scan(lambda h, w: (layer(h, w), None), h, weights)[0]


def reference(x, dy, w_gate, w_up, w_down, m_w_gate, m_w_up, m_w_down, v_w_gate, v_w_up, v_w_down):
    weights = dict(zip(NAMES, (w_gate, w_up, w_down), strict=True))

    def take(so_far, sequence):
        h, by_y = sequence
        _, back = jax.vjp(lambda w: stack(w, h), weights)
        return jax.tree.map(lambda total, term: total + term.astype(jnp.float32), so_far, back(by_y)[0]), None

    none_yet = {name: jnp.zeros(w.shape, jnp.float32) for name, w in weights.items()}
    by_weights, _ = lax.scan(take, none_yet, (x, dy))
    gradients = [by_weights[name].astype(jnp.bfloat16).astype(jnp.float32) for name in NAMES]
    gradients = clipped(gradients, sum(jnp.sum(g * g) for g in gradients), sum(g.size for g in gradients))
    new = [
        adamw(w.astype(jnp.float32), m, v, g)
        for w, m, v, g in zip((w_gate, w_up, w_down), (m_w_gate, m_w_up, m_w_down), (v_w_gate, v_w_up, v_w_down), gradients, strict=True)
    ]
    return tuple(one[which] for which in range(3) for one in new)
```

```python
import functools

import jax
import jax.numpy as jnp
from jax import lax
from jax.experimental import pallas as pl
from jax.experimental.pallas import tpu as pltpu
from jax.sharding import PartitionSpec as P

NAMES = ("w_gate", "w_up", "w_down")
BF, F32 = jnp.bfloat16, jnp.float32
MESH = pl.DeviceIdType.MESH
VMEM, ANY, DMA = pltpu.VMEM, pl.ANY, pltpu.SemaphoreType.DMA

T, D, FF = 4096, 896, 2304
HALF = FF // 2
C = 256
N = FF // C
TB = 512
NT = T // TB
SLOTS = 4
GROUPS = NT // SLOTS
RB = 256


def dot(a, b, ca=1, cb=0):
    return lax.dot_general(a, b, (((ca,), (cb,)), ((), ())), preferred_element_type=F32)


def rows(i, n):
    return pl.ds(pl.multiple_of(i * n, n), n)


def norm_scale(wide):
    return lax.rsqrt(jnp.mean(wide * wide, -1, keepdims=True) + 1e-6)


def norm_in_place(ref):
    def body(i, _):
        wide = ref[rows(i, RB), :].astype(F32)
        ref[rows(i, RB), :] = (wide * norm_scale(wide)).astype(BF)
        return 0

    lax.fori_loop(0, T // RB, body, 0)


def zero(ref):
    def body(i, _):
        ref[rows(i, RB), :] = jnp.zeros((RB, D), F32)
        return 0

    lax.fori_loop(0, T // RB, body, 0)


def chunk_copies(j, slot, wg, wu, wd, bg, bu, bd, sem, which=(0, 1, 2)):
    out = []
    for half in range(2):
        at = pl.multiple_of(half * HALF + j * 128, 128)
        if 0 in which:
            out.append(pltpu.make_async_copy(wg.at[:, pl.ds(at, 128)], bg.at[slot, :, pl.ds(half * 128, 128)], sem.at[slot, half]))
        if 1 in which:
            out.append(pltpu.make_async_copy(wu.at[:, pl.ds(at, 128)], bu.at[slot, :, pl.ds(half * 128, 128)], sem.at[slot, 2 + half]))
        if 2 in which:
            out.append(pltpu.make_async_copy(wd.at[pl.ds(at, 128), :], bd.at[slot, pl.ds(half * 128, 128), :], sem.at[slot, 4 + half]))
    return out


def forward_kernel(x_ref, wg, wu, wd, h_ref, kept, a, acc, bg, bu, bd, keep, wsem, ksem, xsem):
    load = pltpu.make_async_copy(x_ref, a, xsem)
    load.start()
    weights = lambda j, slot: chunk_copies(j, slot, wg, wu, wd, bg, bu, bd, wsem)
    for copy in weights(0, 0):
        copy.start()
    load.wait()
    norm_in_place(a)
    zero(acc)

    def keep_copies(kk):
        bank = lax.rem(kk, 2)
        return [
            pltpu.make_async_copy(
                keep.at[bank, n], kept.at[kk // GROUPS, :, rows(lax.rem(kk, GROUPS) * SLOTS + n, TB), :], ksem.at[bank, n]
            )
            for n in range(SLOTS)
        ]

    def step(j, _):
        slot = lax.rem(j, 2)

        @pl.when(j + 1 < N)
        def _():
            for copy in weights(j + 1, 1 - slot):
                copy.start()

        for copy in weights(j, slot):
            copy.wait()

        def some(k, _):
            kk = j * GROUPS + k

            @pl.when(kk >= 2)
            def _():
                for copy in keep_copies(kk - 2):
                    copy.wait()

            bank = lax.rem(kk, 2)
            for n in range(SLOTS):
                s = rows(k * SLOTS + n, TB)
                at = a[s, :]
                gate, up = dot(at, bg[slot]), dot(at, bu[slot])
                keep[bank, n, 0] = gate
                keep[bank, n, 1] = up
                p = (gate * (1 / (1 + jnp.exp(-gate))) * up).astype(BF)
                acc[s, :] += dot(p, bd[slot])
            for copy in keep_copies(kk):
                copy.start()
            return 0

        lax.fori_loop(0, GROUPS, some, 0)
        return 0

    lax.fori_loop(0, N, step, 0)
    for kk in range(N * GROUPS - 2, N * GROUPS):
        for copy in keep_copies(jnp.int32(kk)):
            copy.wait()
    load.start()
    load.wait()

    def last(i, _):
        s = rows(i, RB)
        a[s, :] = (a[s, :].astype(F32) + acc[s, :].astype(BF).astype(F32)).astype(BF)
        return 0

    lax.fori_loop(0, T // RB, last, 0)
    out = pltpu.make_async_copy(a, h_ref, xsem)
    out.start()
    out.wait()


def forward(x, wg, wu, wd):
    any_ = pl.BlockSpec(memory_space=ANY)
    return pl.pallas_call(
        forward_kernel,
        in_specs=[any_] * 4,
        out_specs=[any_] * 2,
        out_shape=[jax.ShapeDtypeStruct((T, D), BF), jax.ShapeDtypeStruct((N, 2, T, C), F32)],
        scratch_shapes=[
            VMEM((T, D), BF),
            VMEM((T, D), F32),
            VMEM((2, D, C), BF),
            VMEM((2, D, C), BF),
            VMEM((2, C, D), BF),
            VMEM((2, SLOTS, 2, TB, C), F32),
            DMA((2, 6)),
            DMA((2, SLOTS)),
            DMA,
        ],
        compiler_params=pltpu.CompilerParams(vmem_limit_bytes=66_000_000),
        cost_estimate=pl.CostEstimate(flops=6 * T * D * FF, bytes_accessed=2 * T * FF * 4, transcendentals=0),
        name="forward",
    )(x, wg, wu, wd)


def backward_kernel(
    x_ref, h_ref, dy_ref, kept, wg, wu, wd, wd0,
    ggu, gd, sq_out,
    a, dy, acc, p, dg, du, bg, bu, bd, keep, res, resd,
    s1, s1d, r1, r1d, s2, s2d, own2, own2d, r2, r2d, s3, s3d, own3, own3d, r3, r3d, fin, find, sq, sqr,
    wsem, ksem, xsem, ysem, ssem, rsem, fsem, gsem, dsem, qsend, qrecv,
):
    rep, y, s_ = lax.axis_index("rep"), lax.axis_index("r"), lax.axis_index("s")
    xx, c = s_ // 2, lax.rem(s_, 2)
    at_core = (rep, y, 2 * xx + 1 - c)
    at_x = (rep, y, 2 * (1 - xx) + c)
    at_y = (rep, 1 - y, s_)
    at_diagonal = (rep, 1 - y, 2 * xx + 1 - c)
    me = y * 4 + s_

    barrier = pltpu.get_barrier_semaphore()
    for k in range(1, 8):
        other = lax.rem(me + k, 8)
        pl.semaphore_signal(barrier, inc=1, device_id=(rep, other // 4, lax.rem(other, 4)), device_id_type=MESH)

    weights = lambda j, slot: chunk_copies(j, slot, wg, wu, wd, bg, bu, bd, wsem)
    weights0 = lambda j, slot: chunk_copies(j, slot, wg, wu, wd0, bg, bu, bd, wsem, (2,))
    for copy in weights(0, 0):
        copy.start()
    load_a = pltpu.make_async_copy(h_ref, a, xsem)
    load_x = pltpu.make_async_copy(x_ref, a, xsem)
    load_dy = pltpu.make_async_copy(dy_ref, dy, ysem)
    load_a.start()
    load_dy.start()
    sq[...] = jnp.zeros_like(sq)
    zero(acc)
    load_a.wait()
    norm_in_place(a)
    load_dy.wait()
    pl.semaphore_wait(barrier, 7)

    def remote(src, dst, stage, kind, slot, device):
        return pltpu.make_async_remote_copy(
            src_ref=src, dst_ref=dst, send_sem=ssem.at[stage, kind], recv_sem=rsem.at[stage, kind, slot], device_id=device, device_id_type=MESH
        )

    def exchange1(jj):
        k = lax.rem(jj, 2)
        return remote(s1, r1.at[k], 0, 0, k, at_core), remote(s1d, r1d.at[k], 0, 1, k, at_core)

    def exchange2(jj):
        k = lax.rem(jj, 2)
        return remote(s2, r2.at[k], 1, 0, k, at_x), remote(s2d, r2d.at[k], 1, 1, k, at_x)

    def exchange3(jj):
        k = lax.rem(jj, 2)
        return remote(s3, r3.at[k], 2, 0, k, at_y), remote(s3d, r3d.at[k], 2, 1, k, at_y)

    def go(copies):
        for copy in copies:
            copy.start()

    def done(copies):
        for copy in copies:
            copy.wait()

    def part(which, owner_x, core):
        return pl.ds(pl.multiple_of((2 * owner_x + core) * 224, 32), 224) if which == 0 else pl.ds(pl.multiple_of(owner_x * 128 + core * 64, 64), 64)

    def stage1(jj):
        for q in range(2):
            for g in range(2):
                s1[q, g] = res[g, part(0, q, 1 - c), :].astype(BF)
            s1d[q] = resd[part(1, q, 1 - c), :].astype(BF)
        go(exchange1(jj))

    def stage2(jj):
        k = lax.rem(jj, 2)
        done(exchange1(jj))
        for g in range(2):
            s2[g] = (res[g, part(0, 1 - xx, c), :] + r1[k, 1 - xx, g].astype(F32)).astype(BF)
            own2[g] = res[g, part(0, xx, c), :] + r1[k, xx, g].astype(F32)
        s2d[...] = (resd[part(1, 1 - xx, c), :] + r1d[k, 1 - xx].astype(F32)).astype(BF)
        own2d[...] = resd[part(1, xx, c), :] + r1d[k, xx].astype(F32)
        go(exchange2(jj))

    def stage3(jj):
        k = lax.rem(jj, 2)
        done(exchange2(jj))
        mine, theirs = rows(y, 112), rows(1 - y, 112)
        for g in range(2):
            s3[g] = (own2[g, theirs, :] + r2[k, g, theirs, :].astype(F32)).astype(BF)
            own3[g] = own2[g, mine, :] + r2[k, g, mine, :].astype(F32)
        mine, theirs = rows(y, 32), rows(1 - y, 32)
        s3d[...] = (own2d[theirs, :] + r2d[k, theirs, :].astype(F32)).astype(BF)
        own3d[...] = own2d[mine, :] + r2d[k, mine, :].astype(F32)
        go(exchange3(jj))

    def place(jj):
        return 1 - jj // N, lax.rem(jj, N)

    def finished_gu(jj, far):
        layer, j = place(jj)
        to = ggu.at[layer, j, :, rows(y, 112), :]
        if not far:
            return pltpu.make_async_copy(fin, to, fsem.at[0])
        return pltpu.make_async_remote_copy(src_ref=fin, dst_ref=to, send_sem=fsem.at[1], recv_sem=gsem.at[jj], device_id=at_y, device_id_type=MESH)

    def down_at(jj, core, at):
        layer, j = place(jj)
        first = j * 128 + core * 64
        owner = first // 576
        return owner, gd.at[layer, pl.ds(pl.multiple_of(first - owner * 576 + at * 32, 32), 32), :]

    def finished_d(jj, kind):
        owner, to = down_at(jj, c, y)
        if kind == 3:
            return pltpu.make_async_copy(find, to, fsem.at[2])
        device = (at_core, at_y, at_diagonal)[kind]
        return pltpu.make_async_remote_copy(
            src_ref=find, dst_ref=to, send_sem=fsem.at[3 + kind], recv_sem=dsem.at[kind, jj], device_id=device, device_id_type=MESH
        )

    def sends(jj, act):
        act(finished_gu(jj, False), False)
        act(finished_gu(jj, True), True)
        owner, _ = down_at(jj, c, y)

        @pl.when(owner == c)
        def _():
            act(finished_d(jj, 3), False)
            act(finished_d(jj, 1), True)

        @pl.when(owner != c)
        def _():
            act(finished_d(jj, 0), True)
            act(finished_d(jj, 2), True)

    def start(copy, far):
        copy.start()

    def sent(copy, far):
        copy.wait_send() if far else copy.wait()

    def stage4(jj):
        k = lax.rem(jj, 2)
        done(exchange3(jj))

        @pl.when(jj > 0)
        def _():
            sends(jj - 1, sent)

        total = jnp.zeros((8, 128), F32)
        for g in range(2):
            f = (own3[g] + r3[k, g].astype(F32)).astype(BF)
            fin[g] = f
            f = f.astype(F32)
            total += jnp.sum((f * f).reshape(14, 8, 2, 128), (0, 2))
        f = (own3d[...] + r3d[k].astype(F32)).astype(BF)
        find[...] = f
        f = f.astype(F32)
        total += jnp.sum((f * f).reshape(4, 8, 7, 128), (0, 2))
        sq[...] += total
        sends(jj, start)

    def received(jj):
        finished_gu(jj, True).wait_recv()
        _, j = place(jj)

        @pl.when((2 * j + c) // N == c)
        def _():
            finished_d(jj, 1).wait_recv()

        @pl.when((2 * j + 1 - c) // N == c)
        def _():
            finished_d(jj, 0).wait_recv()
            finished_d(jj, 2).wait_recv()

    def stages(jj):
        @pl.when(jj >= 3)
        def _():
            stage4(jj - 3)

        @pl.when(jj >= 2)
        def _():
            stage3(jj - 2)

        @pl.when(jj >= 1)
        def _():
            stage2(jj - 1)

    def weight_gradients(jj):
        res[0] = dot(a[...], dg[...], 0, 0)
        res[1] = dot(a[...], du[...], 0, 0)
        resd[...] = dot(dy[...], p[...], 0, 0).T
        stage1(jj)

    def silu(gate):
        sigmoid = 1 / (1 + jnp.exp(-gate))
        return gate * sigmoid, sigmoid * (1 + gate * (1 - sigmoid))

    def step1(j, _):
        slot = lax.rem(j, 2)

        @pl.when(j + 1 < N)
        def _():
            go(weights(j + 1, 1 - slot))

        done(weights(j, slot))
        stages(j)

        def some(k, _):
            for n in range(SLOTS):
                s = rows(k * SLOTS + n, TB)
                at = a[s, :]
                gate, up = dot(at, bg[slot]), dot(at, bu[slot])
                dp = dot(dy[s, :], bd[slot], 1, 1).astype(BF).astype(F32)
                silu_, slope = silu(gate)
                p[s, :] = (silu_ * up).astype(BF)
                dgate, dup = (dp * up * slope).astype(BF), (dp * silu_).astype(BF)
                dg[s, :] = dgate
                du[s, :] = dup
                acc[s, :] += dot(dgate, bg[slot], 1, 1) + dot(dup, bu[slot], 1, 1)
            return 0

        lax.fori_loop(0, GROUPS, some, 0)
        weight_gradients(j)
        return 0

    lax.fori_loop(0, N, step1, 0)

    def kept_copies(kk):
        bank = lax.rem(kk, 2)
        return [
            pltpu.make_async_copy(
                kept.at[kk // GROUPS, :, rows(lax.rem(kk, GROUPS) * SLOTS + n, TB), :], keep.at[bank, n], ksem.at[bank, n]
            )
            for n in range(SLOTS)
        ]

    go(kept_copies(jnp.int32(0)) + kept_copies(jnp.int32(1)))
    go(weights0(0, 0))
    load_a.start()
    load_a.wait()

    def between(i, _):
        s = rows(i, RB)
        wide, da = a[s, :].astype(F32), acc[s, :].astype(BF).astype(F32)
        scale = norm_scale(wide)
        inner = jnp.mean(da * wide, -1, keepdims=True)
        back = (da * scale - wide * (scale * scale * scale * inner)).astype(BF).astype(F32)
        dy[s, :] = (dy[s, :].astype(F32) + back).astype(BF)
        return 0

    lax.fori_loop(0, T // RB, between, 0)
    load_x.start()
    load_x.wait()
    norm_in_place(a)

    def step0(j, _):
        slot = lax.rem(j, 2)

        @pl.when(j + 1 < N)
        def _():
            go(weights0(j + 1, 1 - slot))

        done(weights0(j, slot))
        stages(N + j)

        def some(k, _):
            kk = j * GROUPS + k
            bank = lax.rem(kk, 2)
            done(kept_copies(kk))
            for n in range(SLOTS):
                s = rows(k * SLOTS + n, TB)
                dp = dot(dy[s, :], bd[slot], 1, 1).astype(BF).astype(F32)
                gate, up = keep[bank, n, 0], keep[bank, n, 1]
                silu_, slope = silu(gate)
                p[s, :] = (silu_ * up).astype(BF)
                dg[s, :] = (dp * up * slope).astype(BF)
                du[s, :] = (dp * silu_).astype(BF)

            @pl.when(kk + 2 < N * GROUPS)
            def _():
                go(kept_copies(kk + 2))

            return 0

        lax.fori_loop(0, GROUPS, some, 0)
        weight_gradients(N + j)
        return 0

    lax.fori_loop(0, N, step0, 0)
    stage4(2 * N - 3)
    stage3(2 * N - 2)
    stage2(2 * N - 1)
    stage4(2 * N - 2)
    stage3(2 * N - 1)
    stage4(2 * N - 1)

    def square(k):
        other = lax.rem(me + k, 8)
        return pltpu.make_async_remote_copy(
            src_ref=sq, dst_ref=sqr.at[me], send_sem=qsend.at[k - 1], recv_sem=qrecv.at[k - 1],
            device_id=(rep, other // 4, lax.rem(other, 4)), device_id_type=MESH,
        )

    for k in range(1, 8):
        square(k).start()
    sends(2 * N - 1, sent)

    def all_received(jj, _):
        received(jj)
        return 0

    lax.fori_loop(0, 2 * N, all_received, 0)
    for k in range(1, 8):
        came_from = lax.rem(me + 8 - k, 8)
        pltpu.make_async_remote_copy(
            src_ref=sq, dst_ref=sqr.at[came_from], send_sem=qsend.at[k - 1], recv_sem=qrecv.at[k - 1],
            device_id=at_y, device_id_type=MESH,
        ).wait()
    sqr[me] = sq[...]
    sq_out[...] = functools.reduce(lambda t, k: t + sqr[k], range(1, 8), sqr[0])


def backward(x, h, dy, kept, wg, wu, wd, wd0):
    any_ = pl.BlockSpec(memory_space=ANY)
    return pl.pallas_call(
        backward_kernel,
        in_specs=[any_] * 8,
        out_specs=[any_, any_, pl.BlockSpec(memory_space=VMEM)],
        out_shape=[
            jax.ShapeDtypeStruct((2, N, 2, 224, C), BF),
            jax.ShapeDtypeStruct((2, 576, D), BF),
            jax.ShapeDtypeStruct((8, 128), F32),
        ],
        scratch_shapes=[
            VMEM((T, D), BF), VMEM((T, D), BF), VMEM((T, D), F32),
            VMEM((T, C), BF), VMEM((T, C), BF), VMEM((T, C), BF),
            VMEM((2, D, C), BF), VMEM((2, D, C), BF), VMEM((2, C, D), BF),
            VMEM((2, SLOTS, 2, TB, C), F32),
            VMEM((2, D, C), F32), VMEM((C, D), F32),
            VMEM((2, 2, 224, C), BF), VMEM((2, 64, D), BF), VMEM((2, 2, 2, 224, C), BF), VMEM((2, 2, 64, D), BF),
            VMEM((2, 224, C), BF), VMEM((64, D), BF), VMEM((2, 224, C), F32), VMEM((64, D), F32),
            VMEM((2, 2, 224, C), BF), VMEM((2, 64, D), BF),
            VMEM((2, 112, C), BF), VMEM((32, D), BF), VMEM((2, 112, C), F32), VMEM((32, D), F32),
            VMEM((2, 2, 112, C), BF), VMEM((2, 32, D), BF),
            VMEM((2, 112, C), BF), VMEM((32, D), BF), VMEM((8, 128), F32), VMEM((8, 8, 128), F32),
            DMA((2, 6)), DMA((2, SLOTS)), DMA, DMA,
            DMA((3, 2)), DMA((3, 2, 2)), DMA((6,)), DMA((2 * N,)), DMA((3, 2 * N)), DMA((7,)), DMA((7,)),
        ],
        compiler_params=pltpu.CompilerParams(vmem_limit_bytes=66_000_000, collective_id=0, has_side_effects=True),
        cost_estimate=pl.CostEstimate(flops=24 * T * D * FF, bytes_accessed=2 * T * FF * 4, transcendentals=0),
        name="backward",
    )(x, h, dy, kept, wg, wu, wd, wd0)


def adamw(w, m, v, g):
    m = 0.9 * m + 0.1 * g
    v = 0.95 * v + 0.05 * g * g
    step = m * lax.rsqrt(v + 1e-8) + 0.1 * w
    return (w - 0.02 * step).astype(jnp.bfloat16), m, v


def solution(mesh):
    def step(x, dy, *arrays):
        weights, m, v = (arrays[i : i + 3] for i in (0, 3, 6))
        whole = [[lax.all_gather(w[n], "s", axis=0, tiled=True) for w in weights] for n in range(2)]
        h, kept = forward(x[0], *whole[0])
        ggu, gd, squares = backward(x[0], h, dy[0], kept, *whole[1], whole[0][2])
        gu = ggu.reshape(2, N, 2, 224, 2, 128).transpose(2, 0, 3, 4, 1, 5).reshape(2, 2, 224, FF)
        count = 3 * 2 * D * FF
        factor = jnp.minimum(1.0, 0.5 * lax.rsqrt(jnp.sum(squares) / count + 1e-30))
        new = [adamw(w.astype(F32), m, v, g.astype(F32) * factor) for w, m, v, g in zip(weights, m, v, (gu[0], gu[1], gd), strict=True)]
        return tuple(one[which] for which in range(3) for one in new)

    states, cut = P(("rep", "r", "s"), None, None), P(None, "s", None)
    return jax.shard_map(
        step,
        mesh=mesh,
        in_specs=(states, states) + (cut,) * 9,
        out_specs=(P("rep", "s", None),) * 9,
        check_vma=False,
    )
```

```python
import functools

import jax
import jax.numpy as jnp
from jax import lax
from jax.experimental import pallas as pl
from jax.experimental.pallas import tpu as pltpu
from jax.sharding import PartitionSpec as P

BF, F32 = jnp.bfloat16, jnp.float32
MESH = pl.DeviceIdType.MESH
VMEM, ANY, DMA = pltpu.VMEM, pl.ANY, pltpu.SemaphoreType.DMA

T, D, FF = 4096, 896, 2304
HALF = FF // 2
DOWN = 2
C = 256
PAIR, LANES = 2, 128
ROWS, ROWS_Y = 224, 112
UNIT, UNIT_Y = 64, 32
N = FF // C
ALL = PAIR * N
TB = 512
NT = T // TB
SLOTS = 4
GROUPS = NT // SLOTS
GT = SLOTS * TB
RB = 256


def dot(a, b, ca=1, cb=0):
    return lax.dot_general(a, b, (((ca,), (cb,)), ((), ())), preferred_element_type=F32)


def odd(i):
    return lax.rem(i, PAIR)


def rows(i, n):
    return pl.ds(pl.multiple_of(i * n, n), n)


def silu(gate):
    sigmoid = 0.5 * jnp.tanh(0.5 * gate) + 0.5
    value = gate * sigmoid
    return value, sigmoid + value * (1 - sigmoid)


def norm_scale(wide):
    return lax.rsqrt(jnp.mean(wide * wide, -1, keepdims=True) + 1e-6)


def norm_in_place(ref):
    def body(i, _):
        wide = ref[rows(i, RB), :].astype(F32)
        ref[rows(i, RB), :] = (wide * norm_scale(wide)).astype(BF)
        return 0

    lax.fori_loop(0, T // RB, body, 0)


def zero(ref):
    def body(i, _):
        ref[rows(i, RB), :] = jnp.zeros((RB, D), F32)
        return 0

    lax.fori_loop(0, T // RB, body, 0)


def chunk_copies(j, slot, gu, d, bgu, bd, sem):
    out = [pltpu.make_async_copy(d.at[j], bd.at[slot], sem.at[slot, 0])]
    if gu is not None:
        out.append(pltpu.make_async_copy(gu.at[j], bgu.at[slot], sem.at[slot, 1]))
    return out


def go(copies):
    for copy in copies:
        copy.start()


def done(copies):
    for copy in copies:
        copy.wait()


def where():
    rep, y, s = lax.axis_index("rep"), lax.axis_index("r"), lax.axis_index("s")
    x, c = s // 2, odd(s)
    return x, y, c, (rep, y, 2 * x + 1 - c), (rep, y, 2 * (1 - x) + c), (rep, 1 - y, s), (rep, 1 - y, 2 * x + 1 - c)


def forward_kernel(
    x_ref, wg, wu, wd, h_ref, kept, gu1, d1, d0,
    a, acc, gu, d, keep,
    lsem, lsemd, ksem, xsem, ssem, rsem, ssemd, rsemd, osem,
):
    x, y, c, at_core, at_x, at_y, _ = where()
    barrier = pltpu.get_barrier_semaphore()
    for device in (at_core, at_x, at_y):
        pl.semaphore_signal(barrier, inc=1, device_id=device, device_id_type=MESH)

    def block(q, owner_x, core, half=None):
        first = (2 * owner_x + core) * ROWS
        n = ROWS if half is None else ROWS_Y
        if half is not None:
            first = first + half * ROWS_Y
        return gu.at[q, :, pl.ds(pl.multiple_of(first, 16), n), :]

    def block_d(q, owner_x, h, half=None):
        first = owner_x * LANES + h * UNIT
        n = UNIT if half is None else UNIT_Y
        if half is not None:
            first = first + half * UNIT_Y
        return d.at[q, pl.ds(pl.multiple_of(first, UNIT_Y), n), :]

    def own(q):
        layer, j = q // N, lax.rem(q, N)
        out = []
        for g, w in enumerate((wg, wu)):
            for side in range(PAIR):
                at = pl.multiple_of(side * HALF + j * LANES, LANES)
                to = gu.at[q, g, pl.ds(pl.multiple_of((2 * x + c) * ROWS, 16), ROWS), pl.ds(side * LANES, LANES)]
                out.append(pltpu.make_async_copy(w.at[layer, :, pl.ds(at, LANES)], to, lsem.at[q, g, side]))
        return out

    def own_d(q, h):
        layer, j = q // N, lax.rem(q, N)
        at = pl.multiple_of(j * LANES + h * UNIT - c * 576, UNIT)
        return pltpu.make_async_copy(wd.at[layer, pl.ds(at, UNIT), :], block_d(q, x, h), lsemd.at[q, h])

    def holds(q, h, core):
        return (2 * lax.rem(q, N) + h) // N == core

    def each_d(q, core, act):
        for h in range(PAIR):

            @pl.when(holds(q, h, core))
            def _(h=h):
                act(h)

    def remote(ref, kind, q, device):
        return pltpu.make_async_remote_copy(
            src_ref=ref, dst_ref=ref, send_sem=ssem.at[kind, q], recv_sem=rsem.at[kind, q], device_id=device, device_id_type=MESH
        )

    def remote_d(ref, kind, q, h, device):
        return pltpu.make_async_remote_copy(
            src_ref=ref, dst_ref=ref, send_sem=ssemd.at[kind, q, h], recv_sem=rsemd.at[kind, q, h], device_id=device, device_id_type=MESH
        )

    TO = (at_x, at_y, at_core, at_core, at_core)

    def sent(kind, q):
        ref = (block(q, x, c, y), block(q, 1 - x, c, y), block(q, x, c), block(q, 1 - x, c, y), block(q, 1 - x, c, 1 - y))[kind]
        return remote(ref, kind, q, TO[kind])

    def sent_d(kind, q, h):
        ref = (block_d(q, x, h, y), block_d(q, 1 - x, h, y), block_d(q, x, h), block_d(q, 1 - x, h, y), block_d(q, 1 - x, h, 1 - y))[kind]
        return remote_d(ref, kind, q, h, TO[kind])

    def got(kind, q):
        o = 1 - c
        ref = (block(q, 1 - x, c, y), block(q, 1 - x, c, 1 - y), block(q, x, o), block(q, 1 - x, o, y), block(q, 1 - x, o, 1 - y))[kind]
        remote(ref, kind, q, TO[kind]).wait_recv()

    def got_d(kind, q, h):
        ref = (block_d(q, 1 - x, h, y), block_d(q, 1 - x, h, 1 - y), block_d(q, x, h), block_d(q, 1 - x, h, y), block_d(q, 1 - x, h, 1 - y))[kind]
        remote_d(ref, kind, q, h, TO[kind]).wait_recv()

    def send_all(q, _):
        for copy in own(q):
            copy.wait()
        sent(0, q).start()

        def act(h):
            own_d(q, h).wait()
            sent_d(0, q, h).start()

        each_d(q, c, act)
        return 0

    def pass_x(q):
        sent(2, q).start()
        got(0, q)
        sent(1, q).start()
        sent(3, q).start()

        def act(h):
            sent_d(2, q, h).start()
            got_d(0, q, h)
            sent_d(1, q, h).start()
            sent_d(3, q, h).start()

        each_d(q, c, act)

    def pass_y(q):
        got(1, q)
        sent(4, q).start()

        def act(h):
            got_d(1, q, h)
            sent_d(4, q, h).start()

        each_d(q, c, act)

    def ready(q):
        for kind in (2, 3, 4):
            got(kind, q)

        def act(h):
            for kind in (2, 3, 4):
                got_d(kind, q, h)

        each_d(q, 1 - c, act)

    def load_own(q, _):
        go(own(q))
        each_d(q, c, lambda h: own_d(q, h).start())
        return 0

    lax.fori_loop(0, ALL, load_own, 0)
    load = pltpu.make_async_copy(x_ref, a, xsem)
    load.start()
    pl.semaphore_wait(barrier, 3)
    lax.fori_loop(0, ALL, send_all, 0)
    zero(acc)
    load.wait()
    norm_in_place(a)
    pass_x(jnp.int32(0))
    pass_y(jnp.int32(0))

    def keep_copies(kk):
        bank = odd(kk)
        return [
            pltpu.make_async_copy(
                keep.at[bank, n], kept.at[kk // GROUPS, :, rows(lax.rem(kk, GROUPS) * SLOTS + n, TB), :], ksem.at[bank, n]
            )
            for n in range(SLOTS)
        ]

    last_chunk = ALL - 1
    save_d0 = pltpu.make_async_copy(d.at[pl.ds(0, N)], d0, osem.at[0, N])

    def saves(q):
        return [pltpu.make_async_copy(whole.at[q], to.at[q - N], osem.at[i, q - N]) for i, (whole, to) in enumerate(((gu, gu1), (d, d1)))]

    def step(j, _):
        ready(j)

        def some(k, _):
            kk = j * GROUPS + k

            @pl.when(kk < last_chunk)
            def _():
                pass_x(kk + 1)

            @pl.when(kk == 1)
            def _():
                pass_y(kk)

            @pl.when(kk >= 3)
            def _():
                pass_y(kk - 1)

            @pl.when(kk >= N + 2)
            def _():
                ready(kk - 2)
                go(saves(kk - 2))

            @pl.when(kk == last_chunk)
            def _():
                save_d0.start()

            @pl.when(kk >= 2)
            def _():
                done(keep_copies(kk - 2))

            bank = odd(kk)
            for n in range(SLOTS):
                s = rows(k * SLOTS + n, TB)
                at = a[s, :]
                gate, up = dot(at, gu[j, 0]), dot(at, gu[j, 1])
                keep[bank, n, 0] = gate
                keep[bank, n, 1] = up
                p = (silu(gate)[0] * up).astype(BF)
                acc[s, :] += dot(p, d[j])
            go(keep_copies(kk))
            return 0

        lax.fori_loop(0, GROUPS, some, 0)
        return 0

    lax.fori_loop(0, N, step, 0)
    load.start()
    pass_y(jnp.int32(last_chunk))
    load.wait()

    def last(i, _):
        s = rows(i, RB)
        a[s, :] = (a[s, :].astype(F32) + acc[s, :].astype(BF).astype(F32)).astype(BF)
        return 0

    lax.fori_loop(0, T // RB, last, 0)
    out = pltpu.make_async_copy(a, h_ref, xsem)
    out.start()

    for q in (last_chunk - 1, last_chunk):
        ready(jnp.int32(q))
        go(saves(jnp.int32(q)))

    def all_sent(q, _):
        for kind in range(5):
            sent(kind, q).wait_send()

        def act(h):
            for kind in range(5):
                sent_d(kind, q, h).wait_send()

        each_d(q, c, act)
        return 0

    lax.fori_loop(0, ALL, all_sent, 0)
    for kk in range(N * GROUPS - 2, N * GROUPS):
        done(keep_copies(jnp.int32(kk)))
    done((out, save_d0))

    def all_saved(q, _):
        done(saves(q))
        return 0

    lax.fori_loop(N, ALL, all_saved, 0)


def forward(x, wg, wu, wd):
    any_ = pl.BlockSpec(memory_space=ANY)
    return pl.pallas_call(
        forward_kernel,
        in_specs=[any_] * 4,
        out_specs=[any_] * 5,
        out_shape=[
            jax.ShapeDtypeStruct((T, D), BF),
            jax.ShapeDtypeStruct((N, 2, T, C), F32),
            jax.ShapeDtypeStruct((N, 2, D, C), BF),
            jax.ShapeDtypeStruct((N, C, D), BF),
            jax.ShapeDtypeStruct((N, C, D), BF),
        ],
        scratch_shapes=[
            VMEM((T, D), BF),
            VMEM((T, D), F32),
            VMEM((ALL, 2, D, C), BF),
            VMEM((ALL, C, D), BF),
            VMEM((PAIR, SLOTS, 2, TB, C), F32),
            DMA((ALL, 2, 2)), DMA((ALL, 2)), DMA((PAIR, SLOTS)), DMA,
            DMA((5, ALL)), DMA((5, ALL)), DMA((5, ALL, 2)), DMA((5, ALL, 2)), DMA((PAIR, N + 1)),
        ],
        compiler_params=pltpu.CompilerParams(vmem_limit_bytes=66_000_000, collective_id=1, has_side_effects=True),
        cost_estimate=pl.CostEstimate(flops=6 * T * D * FF, bytes_accessed=2 * T * FF * 4, transcendentals=0),
        name="forward",
    )(x, wg, wu, wd)


def backward_kernel(
    x_ref, h_ref, dy_ref, kept, gu1, d1, d0,
    ggu, gd, sq_out,
    a, dy, acc, p0, dg0, du0, p1, dg1, du1, bgu, bd, keep, res, resd,
    s1, s1d, r1, r1d, s2, s2d, own2, own2d, r2, r2d, s3, s3d, own3, own3d, r3, r3d, fin, find, sq, sqr,
    wsem, ksem, xsem, ysem, ssem, rsem, fsem, gsem, dsem, qsend, qrecv,
):
    rep, y, s_ = lax.axis_index("rep"), lax.axis_index("r"), lax.axis_index("s")
    xx, _, c, at_core, at_x, at_y, at_diagonal = where()
    me = y * 4 + s_

    barrier = pltpu.get_barrier_semaphore()
    for k in range(1, 8):
        other = lax.rem(me + k, 8)
        pl.semaphore_signal(barrier, inc=1, device_id=(rep, other // 4, lax.rem(other, 4)), device_id_type=MESH)

    weights = lambda j, slot: chunk_copies(j, slot, gu1, d1, bgu, bd, wsem)
    weights0 = lambda j, slot: chunk_copies(j, slot, None, d0, bgu, bd, wsem)
    for copy in weights(0, 0):
        copy.start()
    load_a = pltpu.make_async_copy(h_ref, a, xsem)
    load_x = pltpu.make_async_copy(x_ref, a, xsem)
    load_dy = pltpu.make_async_copy(dy_ref, dy, ysem)
    load_a.start()
    load_dy.start()
    sq[...] = jnp.zeros_like(sq)
    zero(acc)
    load_a.wait()
    norm_in_place(a)
    load_dy.wait()
    pl.semaphore_wait(barrier, 7)

    def remote(src, dst, stage, kind, slot, device):
        return pltpu.make_async_remote_copy(
            src_ref=src, dst_ref=dst, send_sem=ssem.at[stage, kind], recv_sem=rsem.at[stage, kind, slot], device_id=device, device_id_type=MESH
        )

    def exchange1(jj):
        k = odd(jj)
        return remote(s1, r1.at[k], 0, 0, k, at_core), remote(s1d, r1d.at[k], 0, 1, k, at_core)

    def exchange2(jj):
        k = odd(jj)
        return remote(s2, r2.at[k], 1, 0, k, at_x), remote(s2d, r2d.at[k], 1, 1, k, at_x)

    def exchange3(jj):
        k = odd(jj)
        return remote(s3, r3.at[k], 2, 0, k, at_y), remote(s3d, r3d.at[k], 2, 1, k, at_y)

    def part(which, owner_x, core):
        return pl.ds(pl.multiple_of((2 * owner_x + core) * ROWS, UNIT_Y), ROWS) if which == 0 else pl.ds(pl.multiple_of(owner_x * LANES + core * UNIT, UNIT), UNIT)

    def stage1(jj):
        k = odd(jj)
        for q in range(PAIR):
            for g in range(PAIR):
                s1[q, g] = res[k, g, part(0, q, 1 - c), :].astype(BF)
            s1d[q] = resd[k, part(1, q, 1 - c), :].astype(BF)
        go(exchange1(jj))

    def stage2(jj):
        k = odd(jj)
        done(exchange1(jj))
        for g in range(PAIR):
            s2[g] = (res[k, g, part(0, 1 - xx, c), :] + r1[k, 1 - xx, g].astype(F32)).astype(BF)
            own2[g] = res[k, g, part(0, xx, c), :] + r1[k, xx, g].astype(F32)
        s2d[...] = (resd[k, part(1, 1 - xx, c), :] + r1d[k, 1 - xx].astype(F32)).astype(BF)
        own2d[...] = resd[k, part(1, xx, c), :] + r1d[k, xx].astype(F32)
        go(exchange2(jj))

    def stage3(jj):
        k = odd(jj)
        done(exchange2(jj))
        mine, theirs = rows(y, ROWS_Y), rows(1 - y, ROWS_Y)
        for g in range(PAIR):
            s3[g] = (own2[g, theirs, :] + r2[k, g, theirs, :].astype(F32)).astype(BF)
            own3[g] = own2[g, mine, :] + r2[k, g, mine, :].astype(F32)
        mine, theirs = rows(y, UNIT_Y), rows(1 - y, UNIT_Y)
        s3d[...] = (own2d[theirs, :] + r2d[k, theirs, :].astype(F32)).astype(BF)
        own3d[...] = own2d[mine, :] + r2d[k, mine, :].astype(F32)
        go(exchange3(jj))

    def place(jj):
        return 1 - jj // N, lax.rem(jj, N)

    def finished_gu(jj, far):
        layer, j = place(jj)
        to = ggu.at[layer, j, :, rows(y, ROWS_Y), :]
        if not far:
            return pltpu.make_async_copy(fin, to, fsem.at[0])
        return pltpu.make_async_remote_copy(src_ref=fin, dst_ref=to, send_sem=fsem.at[1], recv_sem=gsem.at[jj], device_id=at_y, device_id_type=MESH)

    def down_at(jj, core, at):
        layer, j = place(jj)
        first = j * LANES + core * UNIT
        owner = first // 576
        return owner, gd.at[layer, pl.ds(pl.multiple_of(first - owner * 576 + at * UNIT_Y, UNIT_Y), UNIT_Y), :]

    def finished_d(jj, kind):
        owner, to = down_at(jj, c, y)
        if kind == 3:
            return pltpu.make_async_copy(find, to, fsem.at[2])
        device = (at_core, at_y, at_diagonal)[kind]
        return pltpu.make_async_remote_copy(
            src_ref=find, dst_ref=to, send_sem=fsem.at[3 + kind], recv_sem=dsem.at[kind, jj], device_id=device, device_id_type=MESH
        )

    def sends(jj, act):
        act(finished_gu(jj, False), False)
        act(finished_gu(jj, True), True)
        owner, _ = down_at(jj, c, y)

        @pl.when(owner == c)
        def _():
            act(finished_d(jj, 3), False)
            act(finished_d(jj, 1), True)

        @pl.when(owner != c)
        def _():
            act(finished_d(jj, 0), True)
            act(finished_d(jj, 2), True)

    def start(copy, far):
        copy.start()

    def sent(copy, far):
        copy.wait_send() if far else copy.wait()

    def stage4(jj):
        k = odd(jj)
        done(exchange3(jj))

        @pl.when(jj > 0)
        def _():
            sends(jj - 1, sent)

        total = jnp.zeros((8, LANES), F32)
        for g in range(PAIR):
            f = (own3[g] + r3[k, g].astype(F32)).astype(BF)
            fin[g] = f
            f = f.astype(F32)
            total += jnp.sum((f * f).reshape(14, 8, 2, LANES), (0, 2))
        f = (own3d[...] + r3d[k].astype(F32)).astype(BF)
        find[...] = f
        f = f.astype(F32)
        total += jnp.sum((f * f).reshape(4, 8, 7, LANES), (0, 2))
        sq[...] += total
        sends(jj, start)

    def received(jj):
        finished_gu(jj, True).wait_recv()
        _, j = place(jj)

        @pl.when((2 * j + c) // N == c)
        def _():
            finished_d(jj, 1).wait_recv()

        @pl.when((2 * j + 1 - c) // N == c)
        def _():
            finished_d(jj, 0).wait_recv()
            finished_d(jj, 2).wait_recv()

    def stages(jj):
        for back, stage in ((4, stage4), (3, stage3), (2, stage2), (1, stage1)):

            @pl.when(jj >= back)
            def _(back=back, stage=stage):
                stage(jj - back)

    banks = ((dg0, du0, p0), (dg1, du1, p1))

    def gradient(which, group, slot):
        left = (dy if which == DOWN else a)[pl.ds(group * GT, GT), :]
        term = dot(left, banks[group][which][...], 0, 0)
        if which == DOWN:
            term = term.T
            resd[slot] = term if group == 0 else resd[slot] + term
        else:
            res[slot, which] = term if group == 0 else res[slot, which] + term

    def clear():
        for ref in banks[1]:
            ref[...] = jnp.zeros((GT, C), BF)

    clear()

    def step1(j, _):
        slot = odd(j)

        @pl.when(j + 1 < N)
        def _():
            go(weights(j + 1, 1 - slot))

        done(weights(j, slot))

        for group in range(GROUPS):
            dg, du, p = banks[group]
            for n in range(SLOTS):
                s, b = pl.ds((group * SLOTS + n) * TB, TB), pl.ds(n * TB, TB)
                at = a[s, :]
                gate, up = dot(at, bgu[slot, 0]), dot(at, bgu[slot, 1])
                dp = dot(dy[s, :], bd[slot], 1, 1).astype(BF).astype(F32)
                if n < 3:
                    gradient(n, 1 - group, slot if group else 1 - slot)
                silu_, slope = silu(gate)
                p[b, :] = (silu_ * up).astype(BF)
                dgate, dup = (dp * up * slope).astype(BF), (dp * silu_).astype(BF)
                dg[b, :] = dgate
                du[b, :] = dup
                acc[s, :] += dot(dgate, bgu[slot, 0], 1, 1) + dot(dup, bgu[slot, 1], 1, 1)
            if group == 0:
                stages(j)
        return 0

    lax.fori_loop(0, N, step1, 0)

    def kept_copies(j, group):
        return [
            pltpu.make_async_copy(kept.at[j, :, pl.ds((group * SLOTS + n) * TB, TB), :], keep.at[group, n], ksem.at[group, n])
            for n in range(SLOTS)
        ]

    go(kept_copies(0, 0) + kept_copies(0, 1))
    for which in range(3):
        gradient(which, 1, (N - 1) % 2)
    clear()
    go(weights0(0, 0))
    load_a.start()
    load_a.wait()

    def between(i, _):
        s = rows(i, RB)
        wide, da = a[s, :].astype(F32), acc[s, :].astype(BF).astype(F32)
        scale = norm_scale(wide)
        inner = jnp.mean(da * wide, -1, keepdims=True)
        back = (da * scale - wide * (scale * scale * scale * inner)).astype(BF).astype(F32)
        dy[s, :] = (dy[s, :].astype(F32) + back).astype(BF)
        return 0

    lax.fori_loop(0, T // RB, between, 0)
    load_x.start()
    load_x.wait()
    norm_in_place(a)

    def step0(j, _):
        slot = odd(j)

        @pl.when(j + 1 < N)
        def _():
            go(weights0(j + 1, 1 - slot))

        done(weights0(j, slot))
        out = lax.rem(N + j, 2)
        for group in range(GROUPS):
            dg, du, p = banks[group]
            done(kept_copies(j, group))
            for n in range(SLOTS):
                s, b = pl.ds((group * SLOTS + n) * TB, TB), pl.ds(n * TB, TB)
                dp = dot(dy[s, :], bd[slot], 1, 1).astype(BF).astype(F32)
                if n < 3:
                    gradient(n, 1 - group, out if group else 1 - out)
                gate, up = keep[group, n, 0], keep[group, n, 1]
                silu_, slope = silu(gate)
                p[b, :] = (silu_ * up).astype(BF)
                dg[b, :] = (dp * up * slope).astype(BF)
                du[b, :] = (dp * silu_).astype(BF)

            @pl.when(j + 1 < N)
            def _(group=group):
                go(kept_copies(j + 1, group))

            if group == 0:
                stages(N + j)
        return 0

    lax.fori_loop(0, N, step0, 0)
    for which in range(3):
        gradient(which, 1, 1)
    end = jnp.int32(ALL - 1)
    stage4(end - 3)
    stage3(end - 2)
    stage2(end - 1)
    stage1(end)
    stage4(end - 2)
    stage3(end - 1)
    stage2(end)
    stage4(end - 1)
    stage3(end)
    stage4(end)

    def square(k):
        other = lax.rem(me + k, 8)
        return pltpu.make_async_remote_copy(
            src_ref=sq, dst_ref=sqr.at[me], send_sem=qsend.at[k - 1], recv_sem=qrecv.at[k - 1],
            device_id=(rep, other // 4, lax.rem(other, 4)), device_id_type=MESH,
        )

    for k in range(1, 8):
        square(k).start()
    sends(end, sent)

    def all_received(jj, _):
        received(jj)
        return 0

    lax.fori_loop(0, ALL, all_received, 0)
    for k in range(1, 8):
        came_from = lax.rem(me + 8 - k, 8)
        pltpu.make_async_remote_copy(
            src_ref=sq, dst_ref=sqr.at[came_from], send_sem=qsend.at[k - 1], recv_sem=qrecv.at[k - 1],
            device_id=at_y, device_id_type=MESH,
        ).wait()
    sqr[me] = sq[...]
    sq_out[...] = functools.reduce(lambda t, k: t + sqr[k], range(1, 8), sqr[0])


def backward(x, h, dy, kept, gu1, d1, d0):
    any_ = pl.BlockSpec(memory_space=ANY)
    return pl.pallas_call(
        backward_kernel,
        in_specs=[any_] * 7,
        out_specs=[any_, any_, pl.BlockSpec(memory_space=VMEM)],
        out_shape=[
            jax.ShapeDtypeStruct((2, N, 2, ROWS, C), BF),
            jax.ShapeDtypeStruct((2, 576, D), BF),
            jax.ShapeDtypeStruct((8, LANES), F32),
        ],
        scratch_shapes=[
            VMEM((T, D), BF), VMEM((T, D), BF), VMEM((T, D), F32),
            *[VMEM((GT, C), BF)] * 6,
            VMEM((PAIR, 2, D, C), BF), VMEM((PAIR, C, D), BF),
            VMEM((PAIR, SLOTS, 2, TB, C), F32),
            VMEM((PAIR, 2, D, C), F32), VMEM((PAIR, C, D), F32),
            VMEM((PAIR, 2, ROWS, C), BF), VMEM((PAIR, UNIT, D), BF), VMEM((PAIR, 2, 2, ROWS, C), BF), VMEM((PAIR, 2, UNIT, D), BF),
            VMEM((PAIR, ROWS, C), BF), VMEM((UNIT, D), BF), VMEM((PAIR, ROWS, C), F32), VMEM((UNIT, D), F32),
            VMEM((PAIR, 2, ROWS, C), BF), VMEM((PAIR, UNIT, D), BF),
            VMEM((PAIR, ROWS_Y, C), BF), VMEM((UNIT_Y, D), BF), VMEM((PAIR, ROWS_Y, C), F32), VMEM((UNIT_Y, D), F32),
            VMEM((PAIR, 2, ROWS_Y, C), BF), VMEM((PAIR, UNIT_Y, D), BF),
            VMEM((PAIR, ROWS_Y, C), BF), VMEM((UNIT_Y, D), BF), VMEM((8, LANES), F32), VMEM((8, 8, LANES), F32),
            DMA((PAIR, 2)), DMA((PAIR, SLOTS)), DMA, DMA,
            DMA((3, 2)), DMA((3, 2, 2)), DMA((6,)), DMA((ALL,)), DMA((3, ALL)), DMA((7,)), DMA((7,)),
        ],
        compiler_params=pltpu.CompilerParams(vmem_limit_bytes=66_000_000, collective_id=0, has_side_effects=True),
        cost_estimate=pl.CostEstimate(flops=24 * T * D * FF, bytes_accessed=2 * T * FF * 4, transcendentals=0),
        name="backward",
    )(x, h, dy, kept, gu1, d1, d0)


def adamw(w, m, v, g):
    m = 0.9 * m + 0.1 * g
    v = 0.95 * v + 0.05 * g * g
    step = m * lax.rsqrt(v + 1e-8) + 0.1 * w
    return (w - 0.02 * step).astype(jnp.bfloat16), m, v


def update_kernel(sq, *refs):
    (wg, wu, wd, mg, mu, md, vg, vu, vd, g0, g1, u0, u1, gd), out = refs[:14], refs[14:]
    mean = jnp.sum(sq[...], keepdims=True) / (3 * 2 * D * FF)
    factor = jnp.minimum(1.0, 0.5 * lax.rsqrt(mean + 1e-30))
    for i, (w, m, v, parts) in enumerate(((wg, mg, vg, (g0, g1)), (wu, mu, vu, (u0, u1)), (wd, md, vd, (gd,)))):
        width = w.shape[-1] // len(parts)
        for n, g in enumerate(parts):
            at = pl.ds(n * width, width)
            new = adamw(w[0, :, at].astype(F32), m[0, :, at], v[0, :, at], g[...].reshape(w.shape[1], width).astype(F32) * factor)
            for which in range(3):
                out[3 * which + i][0, :, at] = new[which]


def update(squares, weights, m, v, ggu, gd):
    wide = pl.BlockSpec((1, ROWS, C), lambda l, q: (l, 0, q))
    tall = pl.BlockSpec((1, 576 // N, D), lambda l, q: (l, q, 0))
    g = lambda which, n: pl.BlockSpec((1, 1, 1, ROWS, LANES), lambda l, q: (l, lax.rem(2 * q + n, N), which, 0, (2 * q + n) // N))
    return pl.pallas_call(
        update_kernel,
        grid=(2, N),
        in_specs=[pl.BlockSpec((8, LANES), lambda l, q: (0, 0))] + [wide, wide, tall] * 3 + [g(0, 0), g(0, 1), g(1, 0), g(1, 1), tall],
        out_specs=[wide, wide, tall] * 3,
        out_shape=[jax.ShapeDtypeStruct(w.shape, t) for t in (BF, F32, F32) for w in weights],
        compiler_params=pltpu.CompilerParams(vmem_limit_bytes=60_000_000),
        name="update",
    )(squares, *weights, *m, *v, ggu, ggu, ggu, ggu, gd)


def solution(mesh):
    def step(x, dy, *arrays):
        weights, m, v = (arrays[i : i + 3] for i in (0, 3, 6))
        h, kept, gu1, d1, d0 = forward(x[0], *weights)
        ggu, gd, squares = backward(x[0], h, dy[0], kept, gu1, d1, d0)
        return tuple(update(squares, weights, m, v, ggu, gd))

    states, cut = P(("rep", "r", "s"), None, None), P(None, "s", None)
    return jax.shard_map(
        step,
        mesh=mesh,
        in_specs=(states, states) + (cut,) * 9,
        out_specs=(P("rep", "s", None),) * 9,
        check_vma=False,
    )
```

```python
import functools

import jax
import jax.numpy as jnp
from jax import lax
from jax.experimental import pallas as pl
from jax.experimental.pallas import tpu as pltpu
from jax.sharding import PartitionSpec as P

BF, F32 = jnp.bfloat16, jnp.float32
MESH = pl.DeviceIdType.MESH
VMEM, ANY, DMA = pltpu.VMEM, pl.ANY, pltpu.SemaphoreType.DMA

T, D, FF = 4096, 896, 2304
HALF = FF // 2
DOWN = 2
C = 256
PAIR, LANES = 2, 128
ROWS, ROWS_Y = 224, 112
UNIT, UNIT_Y = 64, 32
N = FF // C
ALL = PAIR * N
TB = 512
NT = T // TB
SLOTS = 4
GROUPS = NT // SLOTS
GT = SLOTS * TB
RB = 256
EB = 512


def dot(a, b, ca=1, cb=0):
    return lax.dot_general(a, b, (((ca,), (cb,)), ((), ())), preferred_element_type=F32)


def odd(i):
    return lax.rem(i, PAIR)


def rows(i, n):
    return pl.ds(pl.multiple_of(i * n, n), n)


def silu(gate):
    sigmoid = 0.5 * jnp.tanh(0.5 * gate) + 0.5
    value = gate * sigmoid
    return value, sigmoid + value * (1 - sigmoid)


def norm_scale(wide):
    return lax.rsqrt(jnp.mean(wide * wide, -1, keepdims=True) + 1e-6)


def norm_in_place(ref):
    def body(i, _):
        wide = ref[rows(i, RB), :].astype(F32)
        ref[rows(i, RB), :] = (wide * norm_scale(wide)).astype(BF)
        return 0

    lax.fori_loop(0, T // RB, body, 0)


def zero(ref):
    def body(i, _):
        ref[rows(i, RB), :] = jnp.zeros((RB, D), F32)
        return 0

    lax.fori_loop(0, T // RB, body, 0)


def chunk_copies(j, slot, gu, d, bgu, bd, sem):
    out = [pltpu.make_async_copy(d.at[j], bd.at[slot], sem.at[slot, 0])]
    if gu is not None:
        out.append(pltpu.make_async_copy(gu.at[j], bgu.at[slot], sem.at[slot, 1]))
    return out


def go(copies):
    for copy in copies:
        copy.start()


def done(copies):
    for copy in copies:
        copy.wait()


def where():
    rep, y, s = lax.axis_index("rep"), lax.axis_index("r"), lax.axis_index("s")
    x, c = s // 2, odd(s)
    return x, y, c, (rep, y, 2 * x + 1 - c), (rep, y, 2 * (1 - x) + c), (rep, 1 - y, s), (rep, 1 - y, 2 * x + 1 - c)


def forward_kernel(
    x_ref, wg, wu, wd, h_ref, a0_ref, a1_ref, kept, gu1, d1, d0,
    a, acc, gu, d, keep, hb, ab,
    lsem, lsemd, ksem, xsem, ssem, rsem, ssemd, rsemd, osem, hsem,
):
    x, y, c, at_core, at_x, at_y, _ = where()
    barrier = pltpu.get_barrier_semaphore()
    for device in (at_core, at_x, at_y):
        pl.semaphore_signal(barrier, inc=1, device_id=device, device_id_type=MESH)

    def block(q, owner_x, core, half=None):
        first = (2 * owner_x + core) * ROWS
        n = ROWS if half is None else ROWS_Y
        if half is not None:
            first = first + half * ROWS_Y
        return gu.at[q, :, pl.ds(pl.multiple_of(first, 16), n), :]

    def block_d(q, owner_x, h, half=None):
        first = owner_x * LANES + h * UNIT
        n = UNIT if half is None else UNIT_Y
        if half is not None:
            first = first + half * UNIT_Y
        return d.at[q, pl.ds(pl.multiple_of(first, UNIT_Y), n), :]

    def own(q):
        layer, j = q // N, lax.rem(q, N)
        out = []
        for g, w in enumerate((wg, wu)):
            for side in range(PAIR):
                at = pl.multiple_of(side * HALF + j * LANES, LANES)
                to = gu.at[q, g, pl.ds(pl.multiple_of((2 * x + c) * ROWS, 16), ROWS), pl.ds(side * LANES, LANES)]
                out.append(pltpu.make_async_copy(w.at[layer, :, pl.ds(at, LANES)], to, lsem.at[q, g, side]))
        return out

    def own_d(q, h):
        layer, j = q // N, lax.rem(q, N)
        at = pl.multiple_of(j * LANES + h * UNIT - c * 576, UNIT)
        return pltpu.make_async_copy(wd.at[layer, pl.ds(at, UNIT), :], block_d(q, x, h), lsemd.at[q, h])

    def holds(q, h, core):
        return (2 * lax.rem(q, N) + h) // N == core

    def each_d(q, core, act):
        for h in range(PAIR):

            @pl.when(holds(q, h, core))
            def _(h=h):
                act(h)

    def remote(ref, kind, q, device):
        return pltpu.make_async_remote_copy(
            src_ref=ref, dst_ref=ref, send_sem=ssem.at[kind, q], recv_sem=rsem.at[kind, q], device_id=device, device_id_type=MESH
        )

    def remote_d(ref, kind, q, h, device):
        return pltpu.make_async_remote_copy(
            src_ref=ref, dst_ref=ref, send_sem=ssemd.at[kind, q, h], recv_sem=rsemd.at[kind, q, h], device_id=device, device_id_type=MESH
        )

    TO = (at_x, at_y, at_core, at_core, at_core)

    def sent(kind, q):
        ref = (block(q, x, c, y), block(q, 1 - x, c, y), block(q, x, c), block(q, 1 - x, c, y), block(q, 1 - x, c, 1 - y))[kind]
        return remote(ref, kind, q, TO[kind])

    def sent_d(kind, q, h):
        ref = (block_d(q, x, h, y), block_d(q, 1 - x, h, y), block_d(q, x, h), block_d(q, 1 - x, h, y), block_d(q, 1 - x, h, 1 - y))[kind]
        return remote_d(ref, kind, q, h, TO[kind])

    def got(kind, q):
        o = 1 - c
        ref = (block(q, 1 - x, c, y), block(q, 1 - x, c, 1 - y), block(q, x, o), block(q, 1 - x, o, y), block(q, 1 - x, o, 1 - y))[kind]
        remote(ref, kind, q, TO[kind]).wait_recv()

    def got_d(kind, q, h):
        ref = (block_d(q, 1 - x, h, y), block_d(q, 1 - x, h, 1 - y), block_d(q, x, h), block_d(q, 1 - x, h, y), block_d(q, 1 - x, h, 1 - y))[kind]
        remote_d(ref, kind, q, h, TO[kind]).wait_recv()

    def send_all(q, _):
        for copy in own(q):
            copy.wait()
        sent(0, q).start()

        def act(h):
            own_d(q, h).wait()
            sent_d(0, q, h).start()

        each_d(q, c, act)
        return 0

    def pass_x(q):
        sent(2, q).start()
        got(0, q)
        sent(1, q).start()
        sent(3, q).start()

        def act(h):
            sent_d(2, q, h).start()
            got_d(0, q, h)
            sent_d(1, q, h).start()
            sent_d(3, q, h).start()

        each_d(q, c, act)

    def pass_y(q):
        got(1, q)
        sent(4, q).start()

        def act(h):
            got_d(1, q, h)
            sent_d(4, q, h).start()

        each_d(q, c, act)

    def ready(q):
        for kind in (2, 3, 4):
            got(kind, q)

        def act(h):
            for kind in (2, 3, 4):
                got_d(kind, q, h)

        each_d(q, 1 - c, act)

    def load_own(q, _):
        go(own(q))
        each_d(q, c, lambda h: own_d(q, h).start())
        return 0

    lax.fori_loop(0, ALL, load_own, 0)
    load = pltpu.make_async_copy(x_ref, a, xsem)
    load.start()
    pl.semaphore_wait(barrier, 3)
    lax.fori_loop(0, ALL, send_all, 0)
    zero(acc)
    load.wait()
    norm_in_place(a)
    save_a0 = pltpu.make_async_copy(a, a0_ref, osem.at[1, N])
    save_a0.start()
    pass_x(jnp.int32(0))
    pass_y(jnp.int32(0))

    def keep_copies(kk):
        bank = odd(kk)
        return [
            pltpu.make_async_copy(
                keep.at[bank, n], kept.at[kk // GROUPS, :, rows(lax.rem(kk, GROUPS) * SLOTS + n, TB), :], ksem.at[bank, n]
            )
            for n in range(SLOTS)
        ]

    last_chunk = ALL - 1
    save_d0 = pltpu.make_async_copy(d.at[pl.ds(0, N)], d0, osem.at[0, N])

    def saves(q):
        return [pltpu.make_async_copy(whole.at[q], to.at[q - N], osem.at[i, q - N]) for i, (whole, to) in enumerate(((gu, gu1), (d, d1)))]

    def step(j, _):
        ready(j)

        def some(k, _):
            kk = j * GROUPS + k

            @pl.when(kk < last_chunk)
            def _():
                pass_x(kk + 1)

            @pl.when(kk == 1)
            def _():
                pass_y(kk)

            @pl.when(kk >= 3)
            def _():
                pass_y(kk - 1)

            @pl.when(kk >= N + 2)
            def _():
                ready(kk - 2)
                go(saves(kk - 2))

            @pl.when(kk == last_chunk)
            def _():
                save_d0.start()

            @pl.when(kk >= 2)
            def _():
                done(keep_copies(kk - 2))

            bank = odd(kk)
            for n in range(SLOTS):
                s = rows(k * SLOTS + n, TB)
                at = a[s, :]
                gate, up = dot(at, gu[j, 0]), dot(at, gu[j, 1])
                keep[bank, n, 0] = gate
                keep[bank, n, 1] = up
                p = (silu(gate)[0] * up).astype(BF)
                acc[s, :] += dot(p, d[j])
            go(keep_copies(kk))
            return 0

        lax.fori_loop(0, GROUPS, some, 0)
        return 0

    save_a0.wait()
    lax.fori_loop(0, N, step, 0)
    load.start()
    pass_y(jnp.int32(last_chunk))
    load.wait()

    def outs(i):
        k, s = odd(i), rows(i, EB)
        return pltpu.make_async_copy(hb.at[k], h_ref.at[s, :], hsem.at[0, k]), pltpu.make_async_copy(ab.at[k], a1_ref.at[s, :], hsem.at[1, k])

    def last(i, _):
        @pl.when(i >= PAIR)
        def _():
            done(outs(i - PAIR))

        k, s = odd(i), rows(i, EB)
        h = (a[s, :].astype(F32) + acc[s, :].astype(BF).astype(F32)).astype(BF)
        hb[k] = h
        wide = h.astype(F32)
        ab[k] = (wide * norm_scale(wide)).astype(BF)
        go(outs(i))
        return 0

    lax.fori_loop(0, T // EB, last, 0)

    for q in (last_chunk - 1, last_chunk):
        ready(jnp.int32(q))
        go(saves(jnp.int32(q)))

    def all_sent(q, _):
        for kind in range(5):
            sent(kind, q).wait_send()

        def act(h):
            for kind in range(5):
                sent_d(kind, q, h).wait_send()

        each_d(q, c, act)
        return 0

    lax.fori_loop(0, ALL, all_sent, 0)
    for kk in range(N * GROUPS - 2, N * GROUPS):
        done(keep_copies(jnp.int32(kk)))
    save_d0.wait()
    for k in range(PAIR):
        done(outs(jnp.int32(T // EB - PAIR + k)))

    def all_saved(q, _):
        done(saves(q))
        return 0

    lax.fori_loop(N, ALL, all_saved, 0)


def forward(x, wg, wu, wd):
    any_ = pl.BlockSpec(memory_space=ANY)
    return pl.pallas_call(
        forward_kernel,
        in_specs=[any_] * 4,
        out_specs=[any_] * 7,
        out_shape=[
            *[jax.ShapeDtypeStruct((T, D), BF)] * 3,
            jax.ShapeDtypeStruct((N, 2, T, C), F32),
            jax.ShapeDtypeStruct((N, 2, D, C), BF),
            jax.ShapeDtypeStruct((N, C, D), BF),
            jax.ShapeDtypeStruct((N, C, D), BF),
        ],
        scratch_shapes=[
            VMEM((T, D), BF),
            VMEM((T, D), F32),
            VMEM((ALL, 2, D, C), BF),
            VMEM((ALL, C, D), BF),
            VMEM((PAIR, SLOTS, 2, TB, C), F32),
            *[VMEM((PAIR, EB, D), BF)] * 2,
            DMA((ALL, 2, 2)), DMA((ALL, 2)), DMA((PAIR, SLOTS)), DMA,
            DMA((5, ALL)), DMA((5, ALL)), DMA((5, ALL, 2)), DMA((5, ALL, 2)), DMA((PAIR, N + 1)), DMA((PAIR, PAIR)),
        ],
        compiler_params=pltpu.CompilerParams(vmem_limit_bytes=66_000_000, collective_id=1, has_side_effects=True),
        cost_estimate=pl.CostEstimate(flops=6 * T * D * FF, bytes_accessed=2 * T * FF * 4, transcendentals=0),
        name="forward",
    )(x, wg, wu, wd)


def backward_kernel(
    h_ref, a0_ref, a1_ref, dy_ref, kept, gu1, d1, d0,
    ggu, gd, sq_out,
    a, dy, acc, terms, bgu, bd, keep, hb, res, resd,
    s1, s1d, r1, r1d, s2, s2d, own2, own2d, r2, r2d, s3, s3d, own3, own3d, r3, r3d, fin, find, sq, sqr,
    wsem, ksem, hsem, xsem, ysem, ssem, rsem, fsem, gsem, dsem, qsend, qrecv,
):
    rep, y, s_ = lax.axis_index("rep"), lax.axis_index("r"), lax.axis_index("s")
    xx, _, c, at_core, at_x, at_y, at_diagonal = where()
    me = y * 4 + s_

    barrier = pltpu.get_barrier_semaphore()
    for k in range(1, 8):
        other = lax.rem(me + k, 8)
        pl.semaphore_signal(barrier, inc=1, device_id=(rep, other // 4, lax.rem(other, 4)), device_id_type=MESH)

    weights = lambda j, slot: chunk_copies(j, slot, gu1, d1, bgu, bd, wsem)
    weights0 = lambda j, slot: chunk_copies(j, slot, None, d0, bgu, bd, wsem)
    for copy in weights(0, 0):
        copy.start()
    load_a = pltpu.make_async_copy(a1_ref, a, xsem)
    load_a0 = pltpu.make_async_copy(a0_ref, a, xsem)
    load_dy = pltpu.make_async_copy(dy_ref, dy, ysem)
    load_a.start()
    load_dy.start()
    sq[...] = jnp.zeros_like(sq)
    zero(acc)
    load_a.wait()
    load_dy.wait()
    pl.semaphore_wait(barrier, 7)

    def remote(src, dst, stage, kind, slot, device):
        return pltpu.make_async_remote_copy(
            src_ref=src, dst_ref=dst, send_sem=ssem.at[stage, kind], recv_sem=rsem.at[stage, kind, slot], device_id=device, device_id_type=MESH
        )

    def exchange1(jj):
        k = odd(jj)
        return remote(s1, r1.at[k], 0, 0, k, at_core), remote(s1d, r1d.at[k], 0, 1, k, at_core)

    def exchange2(jj):
        k = odd(jj)
        return remote(s2, r2.at[k], 1, 0, k, at_x), remote(s2d, r2d.at[k], 1, 1, k, at_x)

    def exchange3(jj):
        k = odd(jj)
        return remote(s3, r3.at[k], 2, 0, k, at_y), remote(s3d, r3d.at[k], 2, 1, k, at_y)

    def part(which, owner_x, core):
        return pl.ds(pl.multiple_of((2 * owner_x + core) * ROWS, UNIT_Y), ROWS) if which == 0 else pl.ds(pl.multiple_of(owner_x * LANES + core * UNIT, UNIT), UNIT)

    def stage1(jj):
        k = odd(jj)
        for q in range(PAIR):
            for g in range(PAIR):
                s1[q, g] = res[k, g, part(0, q, 1 - c), :].astype(BF)
            s1d[q] = resd[k, part(1, q, 1 - c), :].astype(BF)
        go(exchange1(jj))

    def stage2(jj):
        k = odd(jj)
        done(exchange1(jj))
        for g in range(PAIR):
            s2[g] = (res[k, g, part(0, 1 - xx, c), :] + r1[k, 1 - xx, g].astype(F32)).astype(BF)
            own2[g] = res[k, g, part(0, xx, c), :] + r1[k, xx, g].astype(F32)
        s2d[...] = (resd[k, part(1, 1 - xx, c), :] + r1d[k, 1 - xx].astype(F32)).astype(BF)
        own2d[...] = resd[k, part(1, xx, c), :] + r1d[k, xx].astype(F32)
        go(exchange2(jj))

    def stage3(jj):
        k = odd(jj)
        done(exchange2(jj))
        mine, theirs = rows(y, ROWS_Y), rows(1 - y, ROWS_Y)
        for g in range(PAIR):
            s3[g] = (own2[g, theirs, :] + r2[k, g, theirs, :].astype(F32)).astype(BF)
            own3[g] = own2[g, mine, :] + r2[k, g, mine, :].astype(F32)
        mine, theirs = rows(y, UNIT_Y), rows(1 - y, UNIT_Y)
        s3d[...] = (own2d[theirs, :] + r2d[k, theirs, :].astype(F32)).astype(BF)
        own3d[...] = own2d[mine, :] + r2d[k, mine, :].astype(F32)
        go(exchange3(jj))

    def place(jj):
        return 1 - jj // N, lax.rem(jj, N)

    def finished_gu(jj, far):
        layer, j = place(jj)
        to = ggu.at[layer, j, :, rows(y, ROWS_Y), :]
        if not far:
            return pltpu.make_async_copy(fin, to, fsem.at[0])
        return pltpu.make_async_remote_copy(src_ref=fin, dst_ref=to, send_sem=fsem.at[1], recv_sem=gsem.at[jj], device_id=at_y, device_id_type=MESH)

    def down_at(jj, core, at):
        layer, j = place(jj)
        first = j * LANES + core * UNIT
        owner = first // 576
        return owner, gd.at[layer, pl.ds(pl.multiple_of(first - owner * 576 + at * UNIT_Y, UNIT_Y), UNIT_Y), :]

    def finished_d(jj, kind):
        owner, to = down_at(jj, c, y)
        if kind == 3:
            return pltpu.make_async_copy(find, to, fsem.at[2])
        device = (at_core, at_y, at_diagonal)[kind]
        return pltpu.make_async_remote_copy(
            src_ref=find, dst_ref=to, send_sem=fsem.at[3 + kind], recv_sem=dsem.at[kind, jj], device_id=device, device_id_type=MESH
        )

    def sends(jj, act):
        act(finished_gu(jj, False), False)
        act(finished_gu(jj, True), True)
        owner, _ = down_at(jj, c, y)

        @pl.when(owner == c)
        def _():
            act(finished_d(jj, 3), False)
            act(finished_d(jj, 1), True)

        @pl.when(owner != c)
        def _():
            act(finished_d(jj, 0), True)
            act(finished_d(jj, 2), True)

    def start(copy, far):
        copy.start()

    def sent(copy, far):
        copy.wait_send() if far else copy.wait()

    def stage4(jj):
        k = odd(jj)
        done(exchange3(jj))

        @pl.when(jj > 0)
        def _():
            sends(jj - 1, sent)

        total = jnp.zeros((8, LANES), F32)
        for g in range(PAIR):
            f = (own3[g] + r3[k, g].astype(F32)).astype(BF)
            fin[g] = f
            f = f.astype(F32)
            total += jnp.sum((f * f).reshape(14, 8, 2, LANES), (0, 2))
        f = (own3d[...] + r3d[k].astype(F32)).astype(BF)
        find[...] = f
        f = f.astype(F32)
        total += jnp.sum((f * f).reshape(4, 8, 7, LANES), (0, 2))
        sq[...] += total
        sends(jj, start)

    def received(jj):
        finished_gu(jj, True).wait_recv()
        _, j = place(jj)

        @pl.when((2 * j + c) // N == c)
        def _():
            finished_d(jj, 1).wait_recv()

        @pl.when((2 * j + 1 - c) // N == c)
        def _():
            finished_d(jj, 0).wait_recv()
            finished_d(jj, 2).wait_recv()

    def stages(jj):
        for back, stage in ((4, stage4), (3, stage3), (2, stage2), (1, stage1)):

            @pl.when(jj >= back)
            def _(back=back, stage=stage):
                stage(jj - back)

    def gradient(which, group, slot):
        left = (dy if which == DOWN else a)[rows(group, GT), :]
        term = dot(left, terms[group, which], 0, 0)
        later = group != 0
        if which == DOWN:
            resd[slot] = jnp.where(later, resd[slot], 0.0) + term.T
        else:
            res[slot, which] = jnp.where(later, res[slot, which], 0.0) + term

    def last_gradients(slot):
        for which in (DOWN, 0, 1):
            gradient(which, jnp.int32(1), slot)

    def clear():
        for which in range(3):
            terms[1, which] = jnp.zeros((GT, C), BF)

    clear()

    def step1(j, _):
        slot = odd(j)

        @pl.when(j + 1 < N)
        def _():
            go(weights(j + 1, 1 - slot))

        done(weights(j, slot))

        def some(group, _):
            for n in range(SLOTS):
                s, b = rows(group * SLOTS + n, TB), pl.ds(n * TB, TB)
                at = a[s, :]
                gate, up = dot(at, bgu[slot, 0]), dot(at, bgu[slot, 1])
                dp = dot(dy[s, :], bd[slot], 1, 1).astype(BF).astype(F32)
                if n < 3:
                    gradient(n, 1 - group, odd(slot + 1 + group))
                silu_, slope = silu(gate)
                terms[group, 2, b, :] = (silu_ * up).astype(BF)
                dgate, dup = (dp * up * slope).astype(BF), (dp * silu_).astype(BF)
                terms[group, 0, b, :] = dgate
                terms[group, 1, b, :] = dup
                acc[s, :] += dot(dgate, bgu[slot, 0], 1, 1) + dot(dup, bgu[slot, 1], 1, 1)

            @pl.when(group == 0)
            def _():
                stages(j)

            return 0

        lax.fori_loop(0, GROUPS, some, 0)
        return 0

    lax.fori_loop(0, N, step1, 0)

    def kept_copies(j, group):
        return [
            pltpu.make_async_copy(kept.at[j, :, rows(group * SLOTS + n, TB), :], keep.at[group, n], ksem.at[group, n])
            for n in range(SLOTS)
        ]

    def h_copy(i):
        k = odd(i)
        return pltpu.make_async_copy(h_ref.at[rows(i, EB), :], hb.at[k], hsem.at[k])

    go([h_copy(jnp.int32(k)) for k in range(PAIR)] + kept_copies(0, 0) + kept_copies(0, 1))
    last_gradients((N - 1) % 2)
    load_a0.start()
    clear()
    go(weights0(0, 0))

    def between(i, _):
        k, s = odd(i), rows(i, EB)
        h_copy(i).wait()
        wide, da = hb[k].astype(F32), acc[s, :].astype(BF).astype(F32)
        scale = norm_scale(wide)
        inner = jnp.mean(da * wide, -1, keepdims=True)
        back = (da * scale - wide * (scale * scale * scale * inner)).astype(BF).astype(F32)
        dy[s, :] = (dy[s, :].astype(F32) + back).astype(BF)

        @pl.when(i + PAIR < T // EB)
        def _():
            h_copy(i + PAIR).start()

        return 0

    lax.fori_loop(0, T // EB, between, 0)
    load_a0.wait()

    def step0(j, _):
        slot = odd(j)

        @pl.when(j + 1 < N)
        def _():
            go(weights0(j + 1, 1 - slot))

        done(weights0(j, slot))
        out = lax.rem(N + j, 2)
        def some(group, _):
            done(kept_copies(j, group))
            for n in range(SLOTS):
                s, b = rows(group * SLOTS + n, TB), pl.ds(n * TB, TB)
                dp = dot(dy[s, :], bd[slot], 1, 1).astype(BF).astype(F32)
                if n < 3:
                    gradient(n, 1 - group, odd(out + 1 + group))
                gate, up = keep[group, n, 0], keep[group, n, 1]
                silu_, slope = silu(gate)
                terms[group, 2, b, :] = (silu_ * up).astype(BF)
                terms[group, 0, b, :] = (dp * up * slope).astype(BF)
                terms[group, 1, b, :] = (dp * silu_).astype(BF)

            @pl.when(j + 1 < N)
            def _():
                go(kept_copies(j + 1, group))

            @pl.when(group == 0)
            def _():
                stages(N + j)

            return 0

        lax.fori_loop(0, GROUPS, some, 0)
        return 0

    lax.fori_loop(0, N, step0, 0)
    last_gradients(1)
    end = jnp.int32(ALL - 1)
    stage4(end - 3)
    stage3(end - 2)
    stage2(end - 1)
    stage1(end)
    stage4(end - 2)
    stage3(end - 1)
    stage2(end)
    stage4(end - 1)
    stage3(end)
    stage4(end)

    def square(k):
        other = lax.rem(me + k, 8)
        return pltpu.make_async_remote_copy(
            src_ref=sq, dst_ref=sqr.at[me], send_sem=qsend.at[k - 1], recv_sem=qrecv.at[k - 1],
            device_id=(rep, other // 4, lax.rem(other, 4)), device_id_type=MESH,
        )

    for k in range(1, 8):
        square(k).start()
    sends(end, sent)

    def all_received(jj, _):
        received(jj)
        return 0

    lax.fori_loop(0, ALL, all_received, 0)
    for k in range(1, 8):
        came_from = lax.rem(me + 8 - k, 8)
        pltpu.make_async_remote_copy(
            src_ref=sq, dst_ref=sqr.at[came_from], send_sem=qsend.at[k - 1], recv_sem=qrecv.at[k - 1],
            device_id=at_y, device_id_type=MESH,
        ).wait()
    sqr[me] = sq[...]
    sq_out[...] = functools.reduce(lambda t, k: t + sqr[k], range(1, 8), sqr[0])


def backward(h, a0, a1, dy, kept, gu1, d1, d0):
    any_ = pl.BlockSpec(memory_space=ANY)
    return pl.pallas_call(
        backward_kernel,
        in_specs=[any_] * 8,
        out_specs=[any_, any_, pl.BlockSpec(memory_space=VMEM)],
        out_shape=[
            jax.ShapeDtypeStruct((2, N, 2, ROWS, C), BF),
            jax.ShapeDtypeStruct((2, 576, D), BF),
            jax.ShapeDtypeStruct((8, LANES), F32),
        ],
        scratch_shapes=[
            VMEM((T, D), BF), VMEM((T, D), BF), VMEM((T, D), F32),
            VMEM((GROUPS, 3, GT, C), BF),
            VMEM((PAIR, 2, D, C), BF), VMEM((PAIR, C, D), BF),
            VMEM((PAIR, SLOTS, 2, TB, C), F32),
            VMEM((PAIR, EB, D), BF),
            VMEM((PAIR, 2, D, C), F32), VMEM((PAIR, C, D), F32),
            VMEM((PAIR, 2, ROWS, C), BF), VMEM((PAIR, UNIT, D), BF), VMEM((PAIR, 2, 2, ROWS, C), BF), VMEM((PAIR, 2, UNIT, D), BF),
            VMEM((PAIR, ROWS, C), BF), VMEM((UNIT, D), BF), VMEM((PAIR, ROWS, C), F32), VMEM((UNIT, D), F32),
            VMEM((PAIR, 2, ROWS, C), BF), VMEM((PAIR, UNIT, D), BF),
            VMEM((PAIR, ROWS_Y, C), BF), VMEM((UNIT_Y, D), BF), VMEM((PAIR, ROWS_Y, C), F32), VMEM((UNIT_Y, D), F32),
            VMEM((PAIR, 2, ROWS_Y, C), BF), VMEM((PAIR, UNIT_Y, D), BF),
            VMEM((PAIR, ROWS_Y, C), BF), VMEM((UNIT_Y, D), BF), VMEM((8, LANES), F32), VMEM((8, 8, LANES), F32),
            DMA((PAIR, 2)), DMA((PAIR, SLOTS)), DMA((PAIR,)), DMA, DMA,
            DMA((3, 2)), DMA((3, 2, 2)), DMA((6,)), DMA((ALL,)), DMA((3, ALL)), DMA((7,)), DMA((7,)),
        ],
        compiler_params=pltpu.CompilerParams(vmem_limit_bytes=66_000_000, collective_id=0, has_side_effects=True),
        cost_estimate=pl.CostEstimate(flops=24 * T * D * FF, bytes_accessed=2 * T * FF * 4, transcendentals=0),
        name="backward",
    )(h, a0, a1, dy, kept, gu1, d1, d0)


def adamw(w, m, v, g):
    m = 0.9 * m + 0.1 * g
    v = 0.95 * v + 0.05 * g * g
    step = m * lax.rsqrt(v + 1e-8) + 0.1 * w
    return (w - 0.02 * step).astype(jnp.bfloat16), m, v


def update_kernel(sq, *refs):
    (wg, wu, wd, mg, mu, md, vg, vu, vd, g0, g1, u0, u1, gd), out = refs[:14], refs[14:]
    mean = jnp.sum(sq[...], keepdims=True) / (3 * 2 * D * FF)
    factor = jnp.minimum(1.0, 0.5 * lax.rsqrt(mean + 1e-30))
    for i, (w, m, v, parts) in enumerate(((wg, mg, vg, (g0, g1)), (wu, mu, vu, (u0, u1)), (wd, md, vd, (gd,)))):
        width = w.shape[-1] // len(parts)
        for n, g in enumerate(parts):
            at = pl.ds(n * width, width)
            new = adamw(w[0, :, at].astype(F32), m[0, :, at], v[0, :, at], g[...].reshape(w.shape[1], width).astype(F32) * factor)
            for which in range(3):
                out[3 * which + i][0, :, at] = new[which]


def update(squares, weights, m, v, ggu, gd):
    wide = pl.BlockSpec((1, ROWS, C), lambda l, q: (l, 0, q))
    tall = pl.BlockSpec((1, 576 // N, D), lambda l, q: (l, q, 0))
    g = lambda which, n: pl.BlockSpec((1, 1, 1, ROWS, LANES), lambda l, q: (l, lax.rem(2 * q + n, N), which, 0, (2 * q + n) // N))
    return pl.pallas_call(
        update_kernel,
        grid=(2, N),
        in_specs=[pl.BlockSpec((8, LANES), lambda l, q: (0, 0))] + [wide, wide, tall] * 3 + [g(0, 0), g(0, 1), g(1, 0), g(1, 1), tall],
        out_specs=[wide, wide, tall] * 3,
        out_shape=[jax.ShapeDtypeStruct(w.shape, t) for t in (BF, F32, F32) for w in weights],
        compiler_params=pltpu.CompilerParams(vmem_limit_bytes=60_000_000),
        name="update",
    )(squares, *weights, *m, *v, ggu, ggu, ggu, ggu, gd)


def solution(mesh):
    def step(x, dy, *arrays):
        weights, m, v = (arrays[i : i + 3] for i in (0, 3, 6))
        h, a0, a1, kept, gu1, d1, d0 = forward(x[0], *weights)
        ggu, gd, squares = backward(h, a0, a1, dy[0], kept, gu1, d1, d0)
        return tuple(update(squares, weights, m, v, ggu, gd))

    states, cut = P(("rep", "r", "s"), None, None), P(None, "s", None)
    return jax.shard_map(
        step,
        mesh=mesh,
        in_specs=(states, states) + (cut,) * 9,
        out_specs=(P("rep", "s", None),) * 9,
        check_vma=False,
    )
```

```python
import functools

import jax
import jax.numpy as jnp
from jax import lax
from jax.experimental import pallas as pl
from jax.experimental.pallas import tpu as pltpu
from jax.sharding import PartitionSpec as P

BF, F32 = jnp.bfloat16, jnp.float32
MESH = pl.DeviceIdType.MESH
VMEM, ANY, DMA = pltpu.VMEM, pl.ANY, pltpu.SemaphoreType.DMA

T, D, FF = 4096, 896, 2304
HALF = FF // 2
DOWN = 2
C = 256
PAIR, LANES = 2, 128
ROWS, ROWS_Y = 224, 112
UNIT, UNIT_Y = 64, 32
N = FF // C
ALL = PAIR * N
TB = 512
NT = T // TB
SLOTS = 4
GROUPS = NT // SLOTS
GT = SLOTS * TB
RB = 256
EB = 512


def dot(a, b, ca=1, cb=0):
    return lax.dot_general(a, b, (((ca,), (cb,)), ((), ())), preferred_element_type=F32)


def odd(i):
    return lax.rem(i, PAIR)


def rows(i, n):
    return pl.ds(pl.multiple_of(i * n, n), n)


def silu(gate):
    sigmoid = 0.5 * jnp.tanh(0.5 * gate) + 0.5
    value = gate * sigmoid
    return value, sigmoid + value * (1 - sigmoid)


def norm_scale(wide):
    return lax.rsqrt(jnp.mean(wide * wide, -1, keepdims=True) + 1e-6)


def norm_in_place(ref):
    def body(i, _):
        wide = ref[rows(i, RB), :].astype(F32)
        ref[rows(i, RB), :] = (wide * norm_scale(wide)).astype(BF)
        return 0

    lax.fori_loop(0, T // RB, body, 0)


def zero(ref):
    def body(i, _):
        ref[rows(i, RB), :] = jnp.zeros((RB, D), F32)
        return 0

    lax.fori_loop(0, T // RB, body, 0)


def chunk_copies(j, slot, gu, d, bgu, bd, sem):
    out = [pltpu.make_async_copy(d.at[j], bd.at[slot], sem.at[slot, 0])]
    if gu is not None:
        out.append(pltpu.make_async_copy(gu.at[j], bgu.at[slot], sem.at[slot, 1]))
    return out


def go(copies):
    for copy in copies:
        copy.start()


def done(copies):
    for copy in copies:
        copy.wait()


def where():
    rep, y, s = lax.axis_index("rep"), lax.axis_index("r"), lax.axis_index("s")
    x, c = s // 2, odd(s)
    return x, y, c, (rep, y, 2 * x + 1 - c), (rep, y, 2 * (1 - x) + c), (rep, 1 - y, s), (rep, 1 - y, 2 * x + 1 - c)


def forward_kernel(
    x_ref, wg, wu, wd, h_ref, a0_ref, a1_ref, kept, kept_p, gu1, d1, d0,
    a, acc, gu, d, keep, keep_p, hb, ab,
    lsem, lsemd, ksem, xsem, ssem, rsem, ssemd, rsemd, osem, hsem,
):
    x, y, c, at_core, at_x, at_y, _ = where()
    barrier = pltpu.get_barrier_semaphore()
    for device in (at_core, at_x, at_y):
        pl.semaphore_signal(barrier, inc=1, device_id=device, device_id_type=MESH)

    def block(q, owner_x, core, half=None):
        first = (2 * owner_x + core) * ROWS
        n = ROWS if half is None else ROWS_Y
        if half is not None:
            first = first + half * ROWS_Y
        return gu.at[q, :, pl.ds(pl.multiple_of(first, 16), n), :]

    def block_d(q, owner_x, h, half=None):
        first = owner_x * LANES + h * UNIT
        n = UNIT if half is None else UNIT_Y
        if half is not None:
            first = first + half * UNIT_Y
        return d.at[q, pl.ds(pl.multiple_of(first, UNIT_Y), n), :]

    def own(q):
        layer, j = q // N, lax.rem(q, N)
        out = []
        for g, w in enumerate((wg, wu)):
            for side in range(PAIR):
                at = pl.multiple_of(side * HALF + j * LANES, LANES)
                to = gu.at[q, g, pl.ds(pl.multiple_of((2 * x + c) * ROWS, 16), ROWS), pl.ds(side * LANES, LANES)]
                out.append(pltpu.make_async_copy(w.at[layer, :, pl.ds(at, LANES)], to, lsem.at[q, g, side]))
        return out

    def own_d(q, h):
        layer, j = q // N, lax.rem(q, N)
        at = pl.multiple_of(j * LANES + h * UNIT - c * 576, UNIT)
        return pltpu.make_async_copy(wd.at[layer, pl.ds(at, UNIT), :], block_d(q, x, h), lsemd.at[q, h])

    def holds(q, h, core):
        return (2 * lax.rem(q, N) + h) // N == core

    def each_d(q, core, act):
        for h in range(PAIR):

            @pl.when(holds(q, h, core))
            def _(h=h):
                act(h)

    def remote(ref, kind, q, device):
        return pltpu.make_async_remote_copy(
            src_ref=ref, dst_ref=ref, send_sem=ssem.at[kind, q], recv_sem=rsem.at[kind, q], device_id=device, device_id_type=MESH
        )

    def remote_d(ref, kind, q, h, device):
        return pltpu.make_async_remote_copy(
            src_ref=ref, dst_ref=ref, send_sem=ssemd.at[kind, q, h], recv_sem=rsemd.at[kind, q, h], device_id=device, device_id_type=MESH
        )

    TO = (at_x, at_y, at_core, at_core, at_core)

    def sent(kind, q):
        ref = (block(q, x, c, y), block(q, 1 - x, c, y), block(q, x, c), block(q, 1 - x, c, y), block(q, 1 - x, c, 1 - y))[kind]
        return remote(ref, kind, q, TO[kind])

    def sent_d(kind, q, h):
        ref = (block_d(q, x, h, y), block_d(q, 1 - x, h, y), block_d(q, x, h), block_d(q, 1 - x, h, y), block_d(q, 1 - x, h, 1 - y))[kind]
        return remote_d(ref, kind, q, h, TO[kind])

    def got(kind, q):
        o = 1 - c
        ref = (block(q, 1 - x, c, y), block(q, 1 - x, c, 1 - y), block(q, x, o), block(q, 1 - x, o, y), block(q, 1 - x, o, 1 - y))[kind]
        remote(ref, kind, q, TO[kind]).wait_recv()

    def got_d(kind, q, h):
        ref = (block_d(q, 1 - x, h, y), block_d(q, 1 - x, h, 1 - y), block_d(q, x, h), block_d(q, 1 - x, h, y), block_d(q, 1 - x, h, 1 - y))[kind]
        remote_d(ref, kind, q, h, TO[kind]).wait_recv()

    def send_all(q, _):
        for copy in own(q):
            copy.wait()
        sent(0, q).start()

        def act(h):
            own_d(q, h).wait()
            sent_d(0, q, h).start()

        each_d(q, c, act)
        return 0

    def pass_x(q):
        sent(2, q).start()
        got(0, q)
        sent(1, q).start()
        sent(3, q).start()

        def act(h):
            sent_d(2, q, h).start()
            got_d(0, q, h)
            sent_d(1, q, h).start()
            sent_d(3, q, h).start()

        each_d(q, c, act)

    def pass_y(q):
        got(1, q)
        sent(4, q).start()

        def act(h):
            got_d(1, q, h)
            sent_d(4, q, h).start()

        each_d(q, c, act)

    def ready(q):
        for kind in (2, 3, 4):
            got(kind, q)

        def act(h):
            for kind in (2, 3, 4):
                got_d(kind, q, h)

        each_d(q, 1 - c, act)

    def load_own(q, _):
        go(own(q))
        each_d(q, c, lambda h: own_d(q, h).start())
        return 0

    lax.fori_loop(0, ALL, load_own, 0)
    load = pltpu.make_async_copy(x_ref, a, xsem)
    load.start()
    pl.semaphore_wait(barrier, 3)
    lax.fori_loop(0, ALL, send_all, 0)
    zero(acc)
    load.wait()
    norm_in_place(a)
    save_a0 = pltpu.make_async_copy(a, a0_ref, osem.at[1, N])
    save_a0.start()
    pass_x(jnp.int32(0))
    pass_y(jnp.int32(0))

    def keep_copies(kk):
        bank = odd(kk)
        return [
            pltpu.make_async_copy(
                keep.at[bank, n], kept.at[kk // GROUPS, :, rows(lax.rem(kk, GROUPS) * SLOTS + n, TB), :], ksem.at[bank, n]
            )
            for n in range(SLOTS)
        ] + [pltpu.make_async_copy(keep_p.at[bank], kept_p.at[kk // GROUPS, rows(lax.rem(kk, GROUPS), GT), :], ksem.at[bank, SLOTS])]

    last_chunk = ALL - 1
    save_d0 = pltpu.make_async_copy(d.at[pl.ds(0, N)], d0, osem.at[0, N])

    def saves(q):
        return [pltpu.make_async_copy(whole.at[q], to.at[q - N], osem.at[i, q - N]) for i, (whole, to) in enumerate(((gu, gu1), (d, d1)))]

    def step(j, _):
        ready(j)

        def some(k, _):
            kk = j * GROUPS + k

            @pl.when(kk < last_chunk)
            def _():
                pass_x(kk + 1)

            @pl.when(kk == 1)
            def _():
                pass_y(kk)

            @pl.when(kk >= 3)
            def _():
                pass_y(kk - 1)

            @pl.when(kk >= N + 2)
            def _():
                ready(kk - 2)
                go(saves(kk - 2))

            @pl.when(kk == last_chunk)
            def _():
                save_d0.start()

            @pl.when(kk >= 2)
            def _():
                done(keep_copies(kk - 2))

            bank = odd(kk)

            def products(n):
                at = a[rows(k * SLOTS + n, TB), :]
                return dot(at, gu[j, 0]), dot(at, gu[j, 1])

            ahead = products(0)
            for n in range(SLOTS):
                s = rows(k * SLOTS + n, TB)
                gate, up = ahead
                if n + 1 < SLOTS:
                    ahead = products(n + 1)
                silu_, slope = silu(gate)
                keep[bank, n, 0] = up * slope
                keep[bank, n, 1] = silu_
                p = (silu_ * up).astype(BF)
                keep_p[bank, pl.ds(n * TB, TB), :] = p
                acc[s, :] += dot(p, d[j])
            go(keep_copies(kk))
            return 0

        lax.fori_loop(0, GROUPS, some, 0)
        return 0

    save_a0.wait()
    lax.fori_loop(0, N, step, 0)
    load.start()
    pass_y(jnp.int32(last_chunk))
    load.wait()

    def outs(i):
        k, s = odd(i), rows(i, EB)
        return pltpu.make_async_copy(hb.at[k], h_ref.at[s, :], hsem.at[0, k]), pltpu.make_async_copy(ab.at[k], a1_ref.at[s, :], hsem.at[1, k])

    def last(i, _):
        @pl.when(i >= PAIR)
        def _():
            done(outs(i - PAIR))

        k, s = odd(i), rows(i, EB)
        h = (a[s, :].astype(F32) + acc[s, :].astype(BF).astype(F32)).astype(BF)
        hb[k] = h
        wide = h.astype(F32)
        ab[k] = (wide * norm_scale(wide)).astype(BF)
        go(outs(i))
        return 0

    lax.fori_loop(0, T // EB, last, 0)

    for q in (last_chunk - 1, last_chunk):
        ready(jnp.int32(q))
        go(saves(jnp.int32(q)))

    def all_sent(q, _):
        for kind in range(5):
            sent(kind, q).wait_send()

        def act(h):
            for kind in range(5):
                sent_d(kind, q, h).wait_send()

        each_d(q, c, act)
        return 0

    lax.fori_loop(0, ALL, all_sent, 0)
    for kk in range(N * GROUPS - 2, N * GROUPS):
        done(keep_copies(jnp.int32(kk)))
    save_d0.wait()
    for k in range(PAIR):
        done(outs(jnp.int32(T // EB - PAIR + k)))

    def all_saved(q, _):
        done(saves(q))
        return 0

    lax.fori_loop(N, ALL, all_saved, 0)


def forward(x, wg, wu, wd):
    any_ = pl.BlockSpec(memory_space=ANY)
    return pl.pallas_call(
        forward_kernel,
        in_specs=[any_] * 4,
        out_specs=[any_] * 8,
        out_shape=[
            *[jax.ShapeDtypeStruct((T, D), BF)] * 3,
            jax.ShapeDtypeStruct((N, 2, T, C), F32),
            jax.ShapeDtypeStruct((N, T, C), BF),
            jax.ShapeDtypeStruct((N, 2, D, C), BF),
            jax.ShapeDtypeStruct((N, C, D), BF),
            jax.ShapeDtypeStruct((N, C, D), BF),
        ],
        scratch_shapes=[
            VMEM((T, D), BF),
            VMEM((T, D), F32),
            VMEM((ALL, 2, D, C), BF),
            VMEM((ALL, C, D), BF),
            VMEM((PAIR, SLOTS, 2, TB, C), F32),
            VMEM((PAIR, GT, C), BF),
            *[VMEM((PAIR, EB, D), BF)] * 2,
            DMA((ALL, 2, 2)), DMA((ALL, 2)), DMA((PAIR, SLOTS + 1)), DMA,
            DMA((5, ALL)), DMA((5, ALL)), DMA((5, ALL, 2)), DMA((5, ALL, 2)), DMA((PAIR, N + 1)), DMA((PAIR, PAIR)),
        ],
        compiler_params=pltpu.CompilerParams(vmem_limit_bytes=66_000_000, collective_id=1, has_side_effects=True),
        cost_estimate=pl.CostEstimate(flops=6 * T * D * FF, bytes_accessed=2 * T * FF * 4, transcendentals=0),
        name="forward",
    )(x, wg, wu, wd)


def backward_kernel(
    h_ref, a0_ref, a1_ref, dy_ref, kept, kept_p, gu1, d1, d0,
    ggu, gd, sq_out,
    a, dy, acc, terms, bgu, bd, keep, hb, res, resd,
    s1, s1d, r1, r1d, s2, s2d, own2, own2d, r2, r2d, s3, s3d, own3, own3d, r3, r3d, fin, find, sq, sqr,
    wsem, ksem, hsem, xsem, ysem, ssem, rsem, fsem, gsem, dsem, qsend, qrecv,
):
    rep, y, s_ = lax.axis_index("rep"), lax.axis_index("r"), lax.axis_index("s")
    xx, _, c, at_core, at_x, at_y, at_diagonal = where()
    me = y * 4 + s_

    barrier = pltpu.get_barrier_semaphore()
    for k in range(1, 8):
        other = lax.rem(me + k, 8)
        pl.semaphore_signal(barrier, inc=1, device_id=(rep, other // 4, lax.rem(other, 4)), device_id_type=MESH)

    weights = lambda j, slot: chunk_copies(j, slot, gu1, d1, bgu, bd, wsem)
    weights0 = lambda j, slot: chunk_copies(j, slot, None, d0, bgu, bd, wsem)
    for copy in weights(0, 0):
        copy.start()
    load_a = pltpu.make_async_copy(a1_ref, a, xsem)
    load_a0 = pltpu.make_async_copy(a0_ref, a, xsem)
    load_dy = pltpu.make_async_copy(dy_ref, dy, ysem)
    load_a.start()
    load_dy.start()
    sq[...] = jnp.zeros_like(sq)
    zero(acc)
    load_a.wait()
    load_dy.wait()
    pl.semaphore_wait(barrier, 7)

    def remote(src, dst, stage, kind, slot, device):
        return pltpu.make_async_remote_copy(
            src_ref=src, dst_ref=dst, send_sem=ssem.at[stage, kind], recv_sem=rsem.at[stage, kind, slot], device_id=device, device_id_type=MESH
        )

    def exchange1(jj):
        k = odd(jj)
        return remote(s1, r1.at[k], 0, 0, k, at_core), remote(s1d, r1d.at[k], 0, 1, k, at_core)

    def exchange2(jj):
        k = odd(jj)
        return remote(s2, r2.at[k], 1, 0, k, at_x), remote(s2d, r2d.at[k], 1, 1, k, at_x)

    def exchange3(jj):
        k = odd(jj)
        return remote(s3, r3.at[k], 2, 0, k, at_y), remote(s3d, r3d.at[k], 2, 1, k, at_y)

    def part(which, owner_x, core):
        return pl.ds(pl.multiple_of((2 * owner_x + core) * ROWS, UNIT_Y), ROWS) if which == 0 else pl.ds(pl.multiple_of(owner_x * LANES + core * UNIT, UNIT), UNIT)

    def stage1(jj):
        k = odd(jj)
        for q in range(PAIR):
            for g in range(PAIR):
                s1[q, g] = res[k, g, part(0, q, 1 - c), :].astype(BF)
            s1d[q] = resd[k, part(1, q, 1 - c), :].astype(BF)
        go(exchange1(jj))

    def stage2(jj):
        k = odd(jj)
        done(exchange1(jj))
        for g in range(PAIR):
            s2[g] = (res[k, g, part(0, 1 - xx, c), :] + r1[k, 1 - xx, g].astype(F32)).astype(BF)
            own2[g] = res[k, g, part(0, xx, c), :] + r1[k, xx, g].astype(F32)
        s2d[...] = (resd[k, part(1, 1 - xx, c), :] + r1d[k, 1 - xx].astype(F32)).astype(BF)
        own2d[...] = resd[k, part(1, xx, c), :] + r1d[k, xx].astype(F32)
        go(exchange2(jj))

    def stage3(jj):
        k = odd(jj)
        done(exchange2(jj))
        mine, theirs = rows(y, ROWS_Y), rows(1 - y, ROWS_Y)
        for g in range(PAIR):
            s3[g] = (own2[g, theirs, :] + r2[k, g, theirs, :].astype(F32)).astype(BF)
            own3[g] = own2[g, mine, :] + r2[k, g, mine, :].astype(F32)
        mine, theirs = rows(y, UNIT_Y), rows(1 - y, UNIT_Y)
        s3d[...] = (own2d[theirs, :] + r2d[k, theirs, :].astype(F32)).astype(BF)
        own3d[...] = own2d[mine, :] + r2d[k, mine, :].astype(F32)
        go(exchange3(jj))

    def place(jj):
        return 1 - jj // N, lax.rem(jj, N)

    def finished_gu(jj, far):
        layer, j = place(jj)
        to = ggu.at[layer, j, :, rows(y, ROWS_Y), :]
        if not far:
            return pltpu.make_async_copy(fin, to, fsem.at[0])
        return pltpu.make_async_remote_copy(src_ref=fin, dst_ref=to, send_sem=fsem.at[1], recv_sem=gsem.at[jj], device_id=at_y, device_id_type=MESH)

    def down_at(jj, core, at):
        layer, j = place(jj)
        first = j * LANES + core * UNIT
        owner = first // 576
        return owner, gd.at[layer, pl.ds(pl.multiple_of(first - owner * 576 + at * UNIT_Y, UNIT_Y), UNIT_Y), :]

    def finished_d(jj, kind):
        owner, to = down_at(jj, c, y)
        if kind == 3:
            return pltpu.make_async_copy(find, to, fsem.at[2])
        device = (at_core, at_y, at_diagonal)[kind]
        return pltpu.make_async_remote_copy(
            src_ref=find, dst_ref=to, send_sem=fsem.at[3 + kind], recv_sem=dsem.at[kind, jj], device_id=device, device_id_type=MESH
        )

    def sends(jj, act):
        act(finished_gu(jj, False), False)
        act(finished_gu(jj, True), True)
        owner, _ = down_at(jj, c, y)

        @pl.when(owner == c)
        def _():
            act(finished_d(jj, 3), False)
            act(finished_d(jj, 1), True)

        @pl.when(owner != c)
        def _():
            act(finished_d(jj, 0), True)
            act(finished_d(jj, 2), True)

    def start(copy, far):
        copy.start()

    def sent(copy, far):
        copy.wait_send() if far else copy.wait()

    def stage4(jj):
        k = odd(jj)
        done(exchange3(jj))

        @pl.when(jj > 0)
        def _():
            sends(jj - 1, sent)

        total = jnp.zeros((8, LANES), F32)
        for g in range(PAIR):
            f = (own3[g] + r3[k, g].astype(F32)).astype(BF)
            fin[g] = f
            f = f.astype(F32)
            total += jnp.sum((f * f).reshape(14, 8, 2, LANES), (0, 2))
        f = (own3d[...] + r3d[k].astype(F32)).astype(BF)
        find[...] = f
        f = f.astype(F32)
        total += jnp.sum((f * f).reshape(4, 8, 7, LANES), (0, 2))
        sq[...] += total
        sends(jj, start)

    def received(jj):
        finished_gu(jj, True).wait_recv()
        _, j = place(jj)

        @pl.when((2 * j + c) // N == c)
        def _():
            finished_d(jj, 1).wait_recv()

        @pl.when((2 * j + 1 - c) // N == c)
        def _():
            finished_d(jj, 0).wait_recv()
            finished_d(jj, 2).wait_recv()

    def stages(jj):
        for back, stage in ((4, stage4), (3, stage3), (2, stage2), (1, stage1)):

            @pl.when(jj >= back)
            def _(back=back, stage=stage):
                stage(jj - back)

    def gradient(which, group, slot):
        left = (dy if which == DOWN else a)[rows(group, GT), :]
        term = dot(left, terms[group, which], 0, 0)
        later = group != 0
        if which == DOWN:
            resd[slot] = jnp.where(later, resd[slot], 0.0) + term.T
        else:
            res[slot, which] = jnp.where(later, res[slot, which], 0.0) + term

    def last_gradients(slot):
        for which in (DOWN, 0, 1):
            gradient(which, jnp.int32(1), slot)

    def clear():
        for which in range(3):
            terms[1, which] = jnp.zeros((GT, C), BF)

    clear()

    def step1(j, _):
        slot = odd(j)

        @pl.when(j + 1 < N)
        def _():
            go(weights(j + 1, 1 - slot))

        done(weights(j, slot))

        def some(group, _):
            def products(n):
                s = rows(group * SLOTS + n, TB)
                at = a[s, :]
                return dot(at, bgu[slot, 0]), dot(at, bgu[slot, 1]), dot(dy[s, :], bd[slot], 1, 1)

            ahead = products(0)
            for n in range(SLOTS):
                s, b = rows(group * SLOTS + n, TB), pl.ds(n * TB, TB)
                gate, up, dp = ahead
                dp = dp.astype(BF).astype(F32)
                if n + 1 < SLOTS:
                    ahead = products(n + 1)
                if n < 3:
                    gradient(n, 1 - group, odd(slot + 1 + group))
                silu_, slope = silu(gate)
                terms[group, 2, b, :] = (silu_ * up).astype(BF)
                dgate, dup = (dp * up * slope).astype(BF), (dp * silu_).astype(BF)
                terms[group, 0, b, :] = dgate
                terms[group, 1, b, :] = dup
                acc[s, :] += dot(dgate, bgu[slot, 0], 1, 1) + dot(dup, bgu[slot, 1], 1, 1)

            @pl.when(group == 0)
            def _():
                stages(j)

            return 0

        lax.fori_loop(0, GROUPS, some, 0)
        return 0

    lax.fori_loop(0, N, step1, 0)

    def kept_copies(j, group):
        return [
            pltpu.make_async_copy(kept.at[j, :, rows(group * SLOTS + n, TB), :], keep.at[group, n], ksem.at[group, n])
            for n in range(SLOTS)
        ]

    def h_copy(i):
        k = odd(i)
        return pltpu.make_async_copy(h_ref.at[rows(i, EB), :], hb.at[k], hsem.at[k])

    go([h_copy(jnp.int32(k)) for k in range(PAIR)] + kept_copies(0, 0) + kept_copies(0, 1))
    last_gradients((N - 1) % 2)
    load_a0.start()
    clear()
    go(weights0(0, 0))

    def between(i, _):
        k, s = odd(i), rows(i, EB)
        h_copy(i).wait()
        wide, da = hb[k].astype(F32), acc[s, :].astype(BF).astype(F32)
        scale = norm_scale(wide)
        inner = jnp.mean(da * wide, -1, keepdims=True)
        back = (da * scale - wide * (scale * scale * scale * inner)).astype(BF).astype(F32)
        dy[s, :] = (dy[s, :].astype(F32) + back).astype(BF)

        @pl.when(i + PAIR < T // EB)
        def _():
            h_copy(i + PAIR).start()

        return 0

    lax.fori_loop(0, T // EB, between, 0)
    load_a0.wait()

    def step0(j, _):
        slot = odd(j)

        @pl.when(j + 1 < N)
        def _():
            go(weights0(j + 1, 1 - slot))

        done(weights0(j, slot))
        out = lax.rem(N + j, 2)
        def some(group, _):
            product = pltpu.make_async_copy(kept_p.at[j, rows(group, GT), :], terms.at[group, DOWN], ksem.at[group, SLOTS])
            product.start()
            done(kept_copies(j, group))
            for n in range(SLOTS):
                s, b = rows(group * SLOTS + n, TB), pl.ds(n * TB, TB)
                dp = dot(dy[s, :], bd[slot], 1, 1).astype(BF).astype(F32)
                if n < 3:
                    gradient(n, 1 - group, odd(out + 1 + group))
                terms[group, 0, b, :] = (dp * keep[group, n, 0]).astype(BF)
                terms[group, 1, b, :] = (dp * keep[group, n, 1]).astype(BF)

            product.wait()

            @pl.when(j + 1 < N)
            def _():
                go(kept_copies(j + 1, group))

            @pl.when(group == 0)
            def _():
                stages(N + j)

            return 0

        lax.fori_loop(0, GROUPS, some, 0)
        return 0

    lax.fori_loop(0, N, step0, 0)
    last_gradients(1)
    end = jnp.int32(ALL - 1)
    stage4(end - 3)
    stage3(end - 2)
    stage2(end - 1)
    stage1(end)
    stage4(end - 2)
    stage3(end - 1)
    stage2(end)
    stage4(end - 1)
    stage3(end)
    stage4(end)

    def square(k):
        other = lax.rem(me + k, 8)
        return pltpu.make_async_remote_copy(
            src_ref=sq, dst_ref=sqr.at[me], send_sem=qsend.at[k - 1], recv_sem=qrecv.at[k - 1],
            device_id=(rep, other // 4, lax.rem(other, 4)), device_id_type=MESH,
        )

    for k in range(1, 8):
        square(k).start()
    sends(end, sent)

    def all_received(jj, _):
        received(jj)
        return 0

    lax.fori_loop(0, ALL, all_received, 0)
    for k in range(1, 8):
        came_from = lax.rem(me + 8 - k, 8)
        pltpu.make_async_remote_copy(
            src_ref=sq, dst_ref=sqr.at[came_from], send_sem=qsend.at[k - 1], recv_sem=qrecv.at[k - 1],
            device_id=at_y, device_id_type=MESH,
        ).wait()
    sqr[me] = sq[...]
    sq_out[...] = functools.reduce(lambda t, k: t + sqr[k], range(1, 8), sqr[0])


def backward(h, a0, a1, dy, kept, kept_p, gu1, d1, d0):
    any_ = pl.BlockSpec(memory_space=ANY)
    return pl.pallas_call(
        backward_kernel,
        in_specs=[any_] * 9,
        out_specs=[any_, any_, pl.BlockSpec(memory_space=VMEM)],
        out_shape=[
            jax.ShapeDtypeStruct((2, N, 2, ROWS, C), BF),
            jax.ShapeDtypeStruct((2, 576, D), BF),
            jax.ShapeDtypeStruct((8, LANES), F32),
        ],
        scratch_shapes=[
            VMEM((T, D), BF), VMEM((T, D), BF), VMEM((T, D), F32),
            VMEM((GROUPS, 3, GT, C), BF),
            VMEM((PAIR, 2, D, C), BF), VMEM((PAIR, C, D), BF),
            VMEM((PAIR, SLOTS, 2, TB, C), F32),
            VMEM((PAIR, EB, D), BF),
            VMEM((PAIR, 2, D, C), F32), VMEM((PAIR, C, D), F32),
            VMEM((PAIR, 2, ROWS, C), BF), VMEM((PAIR, UNIT, D), BF), VMEM((PAIR, 2, 2, ROWS, C), BF), VMEM((PAIR, 2, UNIT, D), BF),
            VMEM((PAIR, ROWS, C), BF), VMEM((UNIT, D), BF), VMEM((PAIR, ROWS, C), F32), VMEM((UNIT, D), F32),
            VMEM((PAIR, 2, ROWS, C), BF), VMEM((PAIR, UNIT, D), BF),
            VMEM((PAIR, ROWS_Y, C), BF), VMEM((UNIT_Y, D), BF), VMEM((PAIR, ROWS_Y, C), F32), VMEM((UNIT_Y, D), F32),
            VMEM((PAIR, 2, ROWS_Y, C), BF), VMEM((PAIR, UNIT_Y, D), BF),
            VMEM((PAIR, ROWS_Y, C), BF), VMEM((UNIT_Y, D), BF), VMEM((8, LANES), F32), VMEM((8, 8, LANES), F32),
            DMA((PAIR, 2)), DMA((PAIR, SLOTS + 1)), DMA((PAIR,)), DMA, DMA,
            DMA((3, 2)), DMA((3, 2, 2)), DMA((6,)), DMA((ALL,)), DMA((3, ALL)), DMA((7,)), DMA((7,)),
        ],
        compiler_params=pltpu.CompilerParams(vmem_limit_bytes=66_000_000, collective_id=0, has_side_effects=True),
        cost_estimate=pl.CostEstimate(flops=24 * T * D * FF, bytes_accessed=2 * T * FF * 4, transcendentals=0),
        name="backward",
    )(h, a0, a1, dy, kept, kept_p, gu1, d1, d0)


def adamw(w, m, v, g):
    m = 0.9 * m + 0.1 * g
    v = 0.95 * v + 0.05 * g * g
    step = m * lax.rsqrt(v + 1e-8) + 0.1 * w
    return (w - 0.02 * step).astype(jnp.bfloat16), m, v


def update_kernel(sq, *refs):
    (wg, wu, wd, mg, mu, md, vg, vu, vd, g0, g1, u0, u1, gd), out = refs[:14], refs[14:]
    mean = jnp.sum(sq[...], keepdims=True) / (3 * 2 * D * FF)
    factor = jnp.minimum(1.0, 0.5 * lax.rsqrt(mean + 1e-30))
    for i, (w, m, v, parts) in enumerate(((wg, mg, vg, (g0, g1)), (wu, mu, vu, (u0, u1)), (wd, md, vd, (gd,)))):
        width = w.shape[-1] // len(parts)
        for n, g in enumerate(parts):
            at = pl.ds(n * width, width)
            new = adamw(w[0, :, at].astype(F32), m[0, :, at], v[0, :, at], g[...].reshape(w.shape[1], width).astype(F32) * factor)
            for which in range(3):
                out[3 * which + i][0, :, at] = new[which]


def update(squares, weights, m, v, ggu, gd):
    wide = pl.BlockSpec((1, ROWS, C), lambda l, q: (l, 0, q))
    tall = pl.BlockSpec((1, 576 // N, D), lambda l, q: (l, q, 0))
    g = lambda which, n: pl.BlockSpec((1, 1, 1, ROWS, LANES), lambda l, q: (l, lax.rem(2 * q + n, N), which, 0, (2 * q + n) // N))
    return pl.pallas_call(
        update_kernel,
        grid=(2, N),
        in_specs=[pl.BlockSpec((8, LANES), lambda l, q: (0, 0))] + [wide, wide, tall] * 3 + [g(0, 0), g(0, 1), g(1, 0), g(1, 1), tall],
        out_specs=[wide, wide, tall] * 3,
        out_shape=[jax.ShapeDtypeStruct(w.shape, t) for t in (BF, F32, F32) for w in weights],
        compiler_params=pltpu.CompilerParams(vmem_limit_bytes=60_000_000),
        name="update",
    )(squares, *weights, *m, *v, ggu, ggu, ggu, ggu, gd)


def solution(mesh):
    def step(x, dy, *arrays):
        weights, m, v = (arrays[i : i + 3] for i in (0, 3, 6))
        h, a0, a1, kept, kept_p, gu1, d1, d0 = forward(x[0], *weights)
        ggu, gd, squares = backward(h, a0, a1, dy[0], kept, kept_p, gu1, d1, d0)
        return tuple(update(squares, weights, m, v, ggu, gd))

    states, cut = P(("rep", "r", "s"), None, None), P(None, "s", None)
    return jax.shard_map(
        step,
        mesh=mesh,
        in_specs=(states, states) + (cut,) * 9,
        out_specs=(P("rep", "s", None),) * 9,
        check_vma=False,
    )
```
